256 devices in a mesh: member: 32 (over x, z), domain: 8 (over y, core).
Axes of the slice: x: 4, y: 4, z: 8, core: 2. Of those that a mesh axis runs over, the one named last changes fastest.
Arguments:
- starting_tracer_fields: float32 [32, 2, 8, 512, 640], P('member', None, None, 'domain'), may hold values from -6 to 6
- surface_exchange_inputs: float32 [32, 2, 512, 640], P('member', None, 'domain'), may hold values from -4 to 4
- diffusivity: float32 [2, 8], replicated, may hold values from 0.04 to 0.2
- mixing: float32 [2, 7], replicated, may hold values from 0.02 to 0.1
- land_mask: int32 [512, 640], replicated, may hold values 0 or 1
- obs_index: int32 [8, 32, 256], P('domain'), may hold values from 0 to 1279
- obs_count: int32 [8, 32], P('domain'), may hold values from 1 to 256, as said below
- obs_value: float32 [8, 32, 256], P('domain'), may hold values from -8 to 8
- obs_error: float32 [8, 32, 256], P('domain'), may hold values from 1 to 16
Outputs:
- analysis: float32 [32, 2, 8, 512, 640], P('member', None, None, 'domain')
The draws below stay inside these ranges and needn't reach their ends.
Inputs may be any that keep to these rules, and one draw needn't show every extreme that they name: `obs_index`: A cell of the tile's 2 x 640 surface cells, counted row by row. `obs_count`: slots below the count hold observations, the rest are unused; in every domain the last tile holds exactly 256.
All inputs are finite; a program needn't handle non-finite values.
Results may differ from the reference program's by a relative error of at most 0.0001.
Values sent between devices are 32-bit elements; how exact they have to be, the bound alone decides.
No kernel may reach another device: no remote copies, remote signals or barrier semaphores. Data moves between devices by JAX's collectives and lax.ppermute only.
A program may use at most 64 MiB of HBM per device.

```python
import math
import jax
import jax.numpy as jnp
from jax import lax

FIELDS = 2
LEVELS = 8
STEPS = 2
LON = 640
ROWS_TILE = 2
OBS_TILE = 256
MEMBERS = 32
TILES = 32
DOMAINS = 8
SUBREGION_BANDS = 64
LAT = 512


def draw_obs_count(key, part):
    tile_rank = jnp.arange(TILES, dtype=jnp.int32)
    rising = OBS_TILE // 3 + (OBS_TILE - OBS_TILE // 3) * tile_rank // max(TILES - 1, 1)
    jitter = jax.random.randint(jax.random.fold_in(key, 7), (DOMAINS, TILES), 0, OBS_TILE // 6 + 1)
    counts = jnp.clip(rising[None, :] - jitter, 1, OBS_TILE)
    return counts.at[:, TILES - 1].set(OBS_TILE).astype(jnp.int32)


def with_ends(array, own_key, low, high):
    shape = array.shape
    spot = [jax.random.randint(jax.random.fold_in(own_key, axis), (), 0, shape[axis]) for axis in range(len(shape))]
    array = array.at[tuple(spot)].set(low)
    longest = shape.index(max(shape))
    spot[longest] = (spot[longest] + 1) % shape[longest]
    return array.at[tuple(spot)].set(high)


def block_levels(own_key, extent, split, smallest, high):
    loudness = 1.0
    for axis_at, parts in split:
        draws = jax.random.uniform(jax.random.fold_in(jax.random.fold_in(own_key, 6), axis_at), (parts,), jnp.float32, smallest / len(split), high / len(split))
        loudness = loudness * jnp.repeat(jnp.exp(draws), extent[axis_at] // parts).reshape((-1,) + (1,) * (len(extent) - 1 - axis_at))
    return loudness


def normal_values(key, shape, deviation, reach, split=(), kind=jnp.bfloat16):
    entries = jax.random.normal(key, shape, jnp.float32) * deviation
    if len(split) > 0:
        entries = block_levels(key, shape, split, -0.22, 0.18) * entries
    return jnp.clip(entries, min=-reach, max=reach).astype(kind)


def setup_inputs(seed: int = 0) -> dict:
    seeds = jax.random.split(jax.random.key(seed), 10)
    return {
        "starting_tracer_fields": normal_values(seeds[0], (MEMBERS, FIELDS, LEVELS, LAT, LON), 1.0, 6.0, ((0, 32), (3, 8)), jnp.float32),
        "surface_exchange_inputs": normal_values(seeds[1], (MEMBERS, FIELDS, LAT, LON), 0.5, 4.0, ((0, 32), (2, 8)), jnp.float32),
        "diffusivity": jnp.clip(jnp.exp(jax.random.uniform(seeds[2], (FIELDS, LEVELS), jnp.float32, math.log(0.04), math.log(0.2))), 0.04, 0.2),
        "mixing": jnp.clip(jnp.exp(jax.random.uniform(seeds[3], (FIELDS, LEVELS - 1), jnp.float32, math.log(0.02), math.log(0.1))), 0.02, 0.1),
        "land_mask": with_ends((jax.random.randint(seeds[4], (LAT, LON), 0, 5) < 4).astype(jnp.int32), jax.random.fold_in(seeds[4], 1), 0, 1),
        "obs_index": with_ends(jax.random.randint(seeds[5], (DOMAINS, TILES, OBS_TILE), 0, ROWS_TILE * LON), jax.random.fold_in(seeds[5], 1), 0, (ROWS_TILE * LON) - 1).astype(jnp.int32),
        "obs_count": draw_obs_count(jax.random.fold_in(seeds[9], 71), 0),
        "obs_value": normal_values(seeds[7], (DOMAINS, TILES, OBS_TILE), 1.5, 8.0, ((0, 8),), jnp.float32),
        "obs_error": jnp.clip(jnp.exp(math.log(16.0) - 2.7725887 * jax.random.uniform(seeds[8], (DOMAINS, TILES, OBS_TILE), jnp.float32) ** block_levels(seeds[8], (DOMAINS, TILES, OBS_TILE), ((0, 8),), -0.2, 0.2)), 1.0, 16.0),
    }


def stencil(padded, mask_rows, diffusivity, mixing, surface_exchange_inputs):
    middle = padded[:, :, 1:-1]
    mask_mid = mask_rows[1:-1]
    upper_row = padded[:, :, 2:]
    lower_row = padded[:, :, :-2]
    east_cell = jnp.roll(middle, -1, axis=3)
    west_cell = jnp.roll(middle, 1, axis=3)
    lateral = mask_rows[2:] * (upper_row - middle) + mask_rows[:-2] * (lower_row - middle)
    lateral = lateral + jnp.roll(mask_mid, -1, axis=1) * (east_cell - middle)
    lateral = lateral + jnp.roll(mask_mid, 1, axis=1) * (west_cell - middle)
    downward_flux = mixing[:, :, None, None] * (middle[:, 1:] - middle[:, :-1])
    empty_level = jnp.zeros_like(middle[:, :1])
    vertical = jnp.concatenate([downward_flux, empty_level], axis=1) - jnp.concatenate([empty_level, downward_flux], axis=1)
    tendency = diffusivity[:, :, None, None] * lateral + vertical
    tendency = tendency.at[:, 0].add(surface_exchange_inputs)
    return middle + mask_mid * tendency

def partial_sums(observed, values, errors, active):
    average = lax.optimization_barrier(jnp.mean(observed, axis=0))
    anomaly = observed - average[None, :]
    weight_obs = active / errors
    gram = jnp.dot(anomaly * weight_obs[None, :], anomaly.T, precision=lax.Precision.HIGHEST)
    pull = jnp.dot(anomaly, weight_obs * (values - average), precision=lax.Precision.HIGHEST)
    return (gram, pull)

def transform(gram, pull):
    count = gram.shape[0]
    identity = jnp.eye(count, dtype=gram.dtype)
    factor = jnp.linalg.cholesky(gram + (count - 1.0) * identity)
    inverse = jax.scipy.linalg.solve_triangular(factor, identity, lower=True)
    mean_weight = jnp.dot(inverse.T, jnp.dot(inverse, pull, precision=lax.Precision.HIGHEST), precision=lax.Precision.HIGHEST)
    weights = mean_weight[:, None] + jnp.sqrt(count - 1.0) * inverse.T
    return weights - lax.optimization_barrier(jnp.mean(weights, axis=0, keepdims=True)) + 1.0 / count

def reference(starting_tracer_fields, surface_exchange_inputs, diffusivity, mixing, land_mask, obs_index, obs_count, obs_value, obs_error):
    sea_mask = land_mask.astype(jnp.float32)
    padded_mask = jnp.pad(sea_mask, ((1, 1), (0, 0)))

    def predicted_tracer_field(coordinate_couple):
        member_state, member_flux = coordinate_couple
        for _ in range(STEPS):
            padded = jnp.pad(member_state, ((0, 0), (0, 0), (1, 1), (0, 0)))
            member_state = stencil(padded, padded_mask, diffusivity, mixing, member_flux)
        return member_state
    predicted_realisations = lax.map(predicted_tracer_field, (starting_tracer_fields, surface_exchange_inputs))
    count = starting_tracer_fields.shape[0]
    pieces = []
    for subregion_offset in range(DOMAINS):
        subregion_band_slab = predicted_realisations[:, :, :, subregion_offset * SUBREGION_BANDS:(subregion_offset + 1) * SUBREGION_BANDS]
        surface = subregion_band_slab[:, 0, 0].reshape(count, -1)
        position = (jnp.arange(TILES, dtype=jnp.int32)[:, None] * (ROWS_TILE * LON) + obs_index[subregion_offset]).reshape(-1)
        observed = surface[:, position]
        active = (jnp.arange(OBS_TILE, dtype=jnp.int32)[None, :] < obs_count[subregion_offset][:, None]).astype(jnp.float32).reshape(-1)
        gram, pull = partial_sums(observed, obs_value[subregion_offset].reshape(-1), obs_error[subregion_offset].reshape(-1), active)
        kernel = transform(gram, pull)
        updated = jnp.einsum('jm,jn->mn', kernel, subregion_band_slab.reshape(count, -1), precision=lax.Precision.HIGHEST).reshape(subregion_band_slab.shape)
        local_mask = sea_mask[subregion_offset * SUBREGION_BANDS:(subregion_offset + 1) * SUBREGION_BANDS]
        pieces.append(jnp.where(local_mask > 0, updated, subregion_band_slab))
    return jnp.concatenate(pieces, axis=3)
```

```python
import functools

import jax
import jax.numpy as jnp
from jax import lax
from jax.experimental import pallas as pl
from jax.experimental.pallas import tpu as pltpu
from jax.sharding import PartitionSpec as P

FIELDS = 2
LEVELS = 8
LANES = 128
HALO = 2


def stencil_rows(src, dst, first, last, field, mask, crowd, flux, coef):
    lateral, above, below = coef
    vertical = above + below
    top = lax.broadcasted_iota(jnp.int32, above.shape, 0) == 0

    def row(r, _):
        x = src[r]
        sea = mask[pl.ds(r, 1), :]
        wet = sea * x
        width = x.shape[1]
        around = mask[pl.ds(r + 1, 1), :] * src[r + 1] + mask[pl.ds(r - 1, 1), :] * src[r - 1]
        around = around + pltpu.roll(wet, 1, 1) + pltpu.roll(wet, width - 1, 1)
        up = pltpu.roll(x, LEVELS - 1, 0)
        down = pltpu.roll(x, 1, 0)
        source = jnp.where(top, flux[pl.ds(r - 1, 1), :], 0.0)
        change = lateral * around + above * up + below * down
        change = change - (lateral * crowd[pl.ds(r, 1), :] + vertical) * x + source
        dst(r, x + sea * change)
        return 0

    lax.fori_loop(first, last, row, 0, unroll=2)


def forecast_kernel(field, x_ref, before_ref, after_ref, flux_ref, mask_ref, diff_ref, mix_ref,
                    *rest):
    if field == 0:
        index_ref, out_ref, observed_ref, now, later, crowd, flux, surface = rest
    else:
        _, out_ref, now, later, crowd, flux = rest
    rows, width = x_ref.shape[3], x_ref.shape[4]
    tall = rows + 2 * HALO
    blocks = width // LANES
    level = lax.broadcasted_iota(jnp.int32, (LEVELS, width), 0)

    lateral = jnp.zeros((LEVELS, width), jnp.float32)
    above = jnp.zeros((LEVELS, width), jnp.float32)
    below = jnp.zeros((LEVELS, width), jnp.float32)
    for l in range(LEVELS):
        lateral = jnp.where(level == l, diff_ref[field, l], lateral)
        if l < LEVELS - 1:
            above = jnp.where(level == l, mix_ref[field, l], above)
            below = jnp.where(level == l + 1, mix_ref[field, l], below)
    coef = (lateral, above, below)

    sea = mask_ref[1 : tall - 1, :]
    crowd[1 : tall - 1, :] = (
        mask_ref[0 : tall - 2, :] + mask_ref[2:tall, :]
        + pltpu.roll(sea, 1, 1) + pltpu.roll(sea, width - 1, 1)
    )
    flux[0:1, :] = before_ref[field, HALO * LEVELS : HALO * LEVELS + 1, :]
    flux[1 : rows + 1, :] = flux_ref[0, 0]
    flux[rows + 1 : rows + 2, :] = after_ref[field, HALO * LEVELS : HALO * LEVELS + 1, :]
    for h in range(HALO):
        now[h] = before_ref[field, h * LEVELS : (h + 1) * LEVELS, :]
        now[HALO + rows + h] = after_ref[field, h * LEVELS : (h + 1) * LEVELS, :]

    def turn(b, _):
        start = pl.multiple_of(b * 8, 8)
        now[pl.ds(HALO + start, 8)] = jnp.swapaxes(x_ref[0, 0, :, pl.ds(start, 8), :], 0, 1)
        return 0

    lax.fori_loop(0, rows // 8, turn, 0)

    def keep(r, value):
        later[r] = value

    stencil_rows(now, keep, 1, tall - 1, field, mask_ref, crowd, flux, coef)

    def emit(r, value):
        row = r - HALO
        tile = row // 2
        side = row % 2
        for j in range(blocks):
            out_ref[tile, side * blocks + j] = value[:, j * LANES : (j + 1) * LANES]
        if field == 0:
            surface[side, pl.ds(tile, 1), :] = value[0:1, :]

    stencil_rows(later, emit, HALO, HALO + rows, field, mask_ref, crowd, flux, coef)

    if field == 0:
        tiles = rows // 2
        slots = index_ref.shape[2]
        for g in range(tiles // 8):
            for h in range(slots // LANES):
                where = index_ref[0, g * 8 : (g + 1) * 8, h * LANES : (h + 1) * LANES]
                block, lane = where >> 7, where & (LANES - 1)
                found = jnp.zeros((8, LANES), jnp.float32)
                for q in range(2 * blocks):
                    s, j = divmod(q, blocks)
                    source = surface[s, g * 8 : (g + 1) * 8, j * LANES : (j + 1) * LANES]
                    taken = jnp.take_along_axis(source, lane, axis=1, mode="promise_in_bounds")
                    found = jnp.where(block == q, taken, found)
                observed_ref[g * 8 : (g + 1) * 8, h, :] = found


def gram_kernel(tile_ref, seen_ref, value_ref, error_ref, count_ref, _, out_ref):
    tile = tile_ref[0]
    halves = seen_ref.shape[1]
    members = seen_ref.shape[0]
    slot = lax.broadcasted_iota(jnp.int32, (1, LANES), 1)
    total = jnp.zeros((members + 8, members), jnp.float32)
    for h in range(halves):
        seen = seen_ref[:, h, :]
        average = jnp.mean(seen, axis=0, keepdims=True)
        anomaly = seen - average
        span = slice(h * LANES, (h + 1) * LANES)
        own = lax.broadcasted_iota(jnp.int32, (value_ref.shape[1], LANES), 0) == tile
        value = jnp.sum(jnp.where(own, value_ref[0, :, span], 0.0), axis=0, keepdims=True)
        error = jnp.sum(jnp.where(own, error_ref[0, :, span], 0.0), axis=0, keepdims=True)
        active = jnp.where(slot + h * LANES < count_ref[0, tile], 1.0, 0.0)
        weight = active / error
        drift = weight * (value - average)
        left = jnp.concatenate([anomaly * weight, jnp.broadcast_to(drift, (8, LANES))], axis=0)
        total = total + lax.dot_general(
            left, anomaly, (((1,), (1,)), ((), ())),
            precision=lax.Precision.HIGHEST, preferred_element_type=jnp.float32,
        )
    packed = jnp.concatenate([total[g * 8 : (g + 1) * 8] for g in range(4)], axis=1)
    pull = jnp.concatenate([total[members : members + 8]] * 4, axis=1)
    row = lax.broadcasted_iota(jnp.int32, packed.shape, 0)
    lane = lax.broadcasted_iota(jnp.int32, packed.shape, 1)
    corner = (lane >= 16) & (lane < 32)
    packed = jnp.where(corner & (row == 0), pltpu.roll(pull, 16, 1), packed)
    packed = jnp.where(corner & (row == 1), pull, packed)
    out_ref[...] = jnp.broadcast_to(packed[None, None], out_ref.shape)


def ensemble_kernel(packed, wide):
    count = 32
    lane = lax.broadcasted_iota(jnp.int32, (count, LANES), 1)
    row = lax.broadcasted_iota(jnp.int32, (count, LANES), 0)
    gram = jnp.concatenate(
        [packed if g == 0 else pltpu.roll(packed, LANES - g * count, 1) for g in range(4)], axis=0
    )
    pull = jnp.where(
        lane[0:1] < 16,
        pltpu.roll(packed[0:8], LANES - 16, 1)[0:1],
        packed[1:2],
    )
    gram = gram + jnp.where(lane == row, count - 1.0, 0.0)
    columns = [jnp.broadcast_to(gram[:, k : k + 1], (count, LANES)) for k in range(count)]
    work = jnp.where(lane == row, 1.0, 0.0)
    for k in range(count):
        base = (k // 8) * 8
        column = columns[k][base:]
        pivot = jnp.broadcast_to(column[k - base : k - base + 1], (8, LANES))
        scale = lax.rsqrt(pivot)
        scale = scale * (1.5 - 0.5 * pivot * scale * scale)
        head = scale[0:1]
        lead = work[k : k + 1] * head
        column = column * head
        below = row[base:] > k
        factor = jnp.where(below, column, 0.0)
        rest = jnp.where(row[base:] == k, lead, work[base:] - factor * lead)
        work = rest if base == 0 else jnp.concatenate([work[:base], rest], axis=0)
        for c in range(k + 1, count):
            cbase = (c // 8) * 8
            ratio = column[c - base : c - base + 1]
            old = columns[c]
            fresh = old[cbase:] - column[cbase - base :] * ratio
            columns[c] = fresh if cbase == 0 else jnp.concatenate([old[:cbase], fresh], axis=0)
    inverse = work
    gained = jnp.sum(inverse * pull, axis=1, keepdims=True)
    mean_weight = jnp.sum(inverse * gained, axis=0, keepdims=True)
    live = lane < count
    weights = jnp.where(live, mean_weight + jnp.sqrt(count - 1.0) * inverse, 0.0)
    centre = jnp.sum(weights, axis=1, keepdims=True) * (1.0 / count)
    return jnp.where(live, weights - centre + 1.0 / count, 0.0)


def mix_kernel(gram_ref, data_ref, mask_ref, out_ref, high, low):
    members, blocks = data_ref.shape[0], data_ref.shape[1]
    deep = members * LEVELS

    @pl.when(pl.program_id(0) == 0)
    def _():
        kernel = ensemble_kernel(jnp.sum(gram_ref[:, 0], axis=0), LANES)[:, :members]
        major = kernel.astype(jnp.bfloat16)
        minor = (kernel - major.astype(jnp.float32)).astype(jnp.bfloat16)
        spread = (
            lax.broadcasted_iota(jnp.int32, (deep, members), 0) // LEVELS
            == lax.broadcasted_iota(jnp.int32, (deep, members), 1)
        ).astype(jnp.bfloat16)
        same = (
            lax.broadcasted_iota(jnp.int32, (deep, deep), 0) % LEVELS
            == lax.broadcasted_iota(jnp.int32, (deep, deep), 1) % LEVELS
        )
        for part, target in ((major, high), (minor, low)):
            tall = jnp.dot(spread, part, preferred_element_type=jnp.float32).astype(jnp.bfloat16)
            full = lax.dot_general(
                tall, spread, (((1,), (1,)), ((), ())), preferred_element_type=jnp.float32
            )
            target[...] = jnp.where(same, full, 0.0).astype(jnp.bfloat16)

    data = jnp.concatenate([data_ref[:, b].reshape(deep, LANES) for b in range(blocks)], axis=1)
    major = data.astype(jnp.bfloat16)
    minor = (data - major.astype(jnp.float32)).astype(jnp.bfloat16)
    mixed = jnp.dot(high[...], major, preferred_element_type=jnp.float32)
    mixed = mixed + jnp.dot(high[...], minor, preferred_element_type=jnp.float32)
    mixed = mixed + jnp.dot(low[...], major, preferred_element_type=jnp.float32)
    ocean = mask_ref[pl.ds(pl.program_id(0) % 2, 1), :] > 0.0
    mixed = jnp.where(ocean, mixed, data)
    for b in range(blocks):
        out_ref[:, b] = mixed[:, b * LANES : (b + 1) * LANES].reshape(members, LEVELS, LANES)


def settle_kernel(back_ref, out_ref):
    blocks = out_ref.shape[4] // LANES
    for f in range(FIELDS):
        for j in range(blocks):
            rows = []
            for t in range(4):
                for s in range(2):
                    rows.append(back_ref[t, (f * 2 + s) * blocks + j])
            turned = jnp.swapaxes(jnp.stack(rows, axis=0), 0, 1)
            out_ref[0, f, :, :, j * LANES : (j + 1) * LANES] = turned


def shards(
    starting_tracer_fields,
    surface_exchange_inputs,
    diffusivity,
    mixing,
    land_mask,
    obs_index,
    obs_count,
    obs_value,
    obs_error,
):
    _, fields, levels, rows, width = starting_tracer_fields.shape
    members = lax.axis_size("member")
    domains = lax.axis_size("domain")
    blocks = width // LANES
    tiles = members
    per_field = 2 * blocks
    slabs = fields * per_field + 1
    tile = lax.axis_index("member")
    domain = lax.axis_index("domain")
    state, flux = starting_tracer_fields[0], surface_exchange_inputs[0]

    def edge(first, flux_row):
        lines = jnp.swapaxes(state[:, :, first : first + HALO], 1, 2)
        lines = lines.reshape(fields, HALO * levels, width)
        return jnp.concatenate([lines, flux[:, flux_row : flux_row + 1]], axis=1)

    up = [(i, i + 1) for i in range(domains - 1)]
    down = [(i + 1, i) for i in range(domains - 1)]
    before = lax.ppermute(edge(rows - HALO, rows - 1), "domain", up)
    after = lax.ppermute(edge(0, 0), "domain", down)

    padded = jnp.pad(land_mask, ((HALO, HALO), (0, 0)))
    mask = lax.dynamic_slice_in_dim(padded, domain * rows, rows + 2 * HALO, 0).astype(jnp.float32)
    tile_mask = lax.dynamic_slice_in_dim(mask, HALO + tile * 2, 2, 0)

    f32 = jnp.float32
    tall = rows + 2 * HALO
    bulk = jax.ShapeDtypeStruct((tiles, slabs, levels, LANES), f32)

    def whole(*shape):
        return pl.BlockSpec(shape, lambda i: (0,) * len(shape))

    def forecast(field, extra):
        in_specs = [
            pl.BlockSpec((1, 1, levels, rows, width), lambda i: (0, field, 0, 0, 0)),
            whole(fields, HALO * levels + 1, width),
            whole(fields, HALO * levels + 1, width),
            pl.BlockSpec((1, 1, rows, width), lambda i: (0, field, 0, 0)),
            whole(tall, width),
            pl.BlockSpec(memory_space=pltpu.SMEM),
            pl.BlockSpec(memory_space=pltpu.SMEM),
        ]
        out_shape = [bulk]
        out_specs = [pl.BlockSpec((tiles, per_field, levels, LANES), lambda i: (0, field, 0, 0))]
        scratch = [
            pltpu.VMEM((tall, levels, width), f32),
            pltpu.VMEM((tall, levels, width), f32),
            pltpu.VMEM((tall, width), f32),
            pltpu.VMEM((rows + 2, width), f32),
        ]
        alias = {}
        if field == 0:
            in_specs.append(whole(*obs_index.shape))
            slots = obs_index.shape[2]
            out_shape.append(jax.ShapeDtypeStruct((tiles, slots // LANES, LANES), f32))
            out_specs.append(whole(tiles, slots // LANES, LANES))
            scratch.append(pltpu.VMEM((2, tiles, width), f32))
        else:
            in_specs.append(pl.BlockSpec(memory_space=pl.ANY))
            alias = {7: 0}
        return pl.pallas_call(
            functools.partial(forecast_kernel, field),
            grid=(1,),
            out_shape=out_shape,
            in_specs=in_specs,
            out_specs=out_specs,
            scratch_shapes=scratch,
            input_output_aliases=alias,
            cost_estimate=pl.CostEstimate(
                flops=40_000_000, bytes_accessed=3_000_000, transcendentals=0
            ),
            name=f"forecast_{field}",
        )(
            starting_tracer_fields, before, after, surface_exchange_inputs, mask,
            diffusivity, mixing, extra,
        )

    sent, observed = forecast(0, obs_index)
    seen = lax.all_to_all(observed, "member", split_axis=0, concat_axis=0, tiled=True)
    (sent,) = forecast(1, sent)

    sent = pl.pallas_call(
        gram_kernel,
        grid=(1,),
        out_shape=bulk,
        in_specs=[
            pl.BlockSpec(memory_space=pltpu.SMEM),
            whole(*seen.shape),
            whole(*obs_value.shape),
            whole(*obs_error.shape),
            pl.BlockSpec(memory_space=pltpu.SMEM),
            pl.BlockSpec(memory_space=pl.ANY),
        ],
        out_specs=pl.BlockSpec((tiles, 1, levels, LANES), lambda i: (0, slabs - 1, 0, 0)),
        input_output_aliases={5: 0},
        name="gram",
    )(tile.reshape(1).astype(jnp.int32), seen, obs_value, obs_error, obs_count, sent)

    held = lax.all_to_all(sent, "member", split_axis=0, concat_axis=0, tiled=True)

    deep = members * levels
    updated = pl.pallas_call(
        mix_kernel,
        grid=(fields * 2,),
        out_shape=jax.ShapeDtypeStruct((members, slabs - 1, levels, LANES), f32),
        in_specs=[
            pl.BlockSpec((members, 1, levels, LANES), lambda i: (0, slabs - 1, 0, 0)),
            pl.BlockSpec((members, blocks, levels, LANES), lambda i: (0, i, 0, 0)),
            whole(2, width),
        ],
        out_specs=pl.BlockSpec((members, blocks, levels, LANES), lambda i: (0, i, 0, 0)),
        scratch_shapes=[
            pltpu.VMEM((deep, deep), jnp.bfloat16),
            pltpu.VMEM((deep, deep), jnp.bfloat16),
        ],
        name="mix",
    )(held, held, tile_mask)

    back = lax.all_to_all(updated, "member", split_axis=0, concat_axis=0, tiled=True)

    return pl.pallas_call(
        settle_kernel,
        grid=(rows // 8,),
        out_shape=jax.ShapeDtypeStruct(starting_tracer_fields.shape, f32),
        in_specs=[pl.BlockSpec((4, slabs - 1, levels, LANES), lambda i: (i, 0, 0, 0))],
        out_specs=pl.BlockSpec((1, fields, levels, 8, width), lambda i: (0, 0, 0, i, 0)),
        name="settle",
    )(back)


def solution(mesh):
    placed = (
        P("member", None, None, "domain", None),
        P("member", None, "domain", None),
        P(),
        P(),
        P(),
        P("domain", None, None),
        P("domain", None),
        P("domain", None, None),
        P("domain", None, None),
    )
    return jax.shard_map(
        shards,
        mesh=mesh,
        in_specs=placed,
        out_specs=P("member", None, None, "domain", None),
        check_vma=False,
    )
```

```python
import functools

import jax
import jax.numpy as jnp
from jax import lax
from jax.experimental import pallas as pl
from jax.experimental.pallas import tpu as pltpu
from jax.sharding import PartitionSpec as P

FIELDS = 2
LEVELS = 8
LANES = 128
HALO = 2
UNROLL = 6


def stencil_rows(src, dst, first, last, field, mask, crowd, flux, coef):
    lateral, above, below = coef
    vertical = above + below
    top = lax.broadcasted_iota(jnp.int32, above.shape, 0) == 0

    def row(r, _):
        x = src[r]
        sea = mask[pl.ds(r, 1), :]
        wet = sea * x
        width = x.shape[1]
        around = mask[pl.ds(r + 1, 1), :] * src[r + 1] + mask[pl.ds(r - 1, 1), :] * src[r - 1]
        around = around + pltpu.roll(wet, 1, 1) + pltpu.roll(wet, width - 1, 1)
        up = pltpu.roll(x, LEVELS - 1, 0)
        down = pltpu.roll(x, 1, 0)
        source = jnp.where(top, flux[pl.ds(r - 1, 1), :], 0.0)
        change = lateral * around + above * up + below * down
        change = change - (lateral * crowd[pl.ds(r, 1), :] + vertical) * x + source
        dst(r, x + sea * change)
        return 0

    lax.fori_loop(first, last, row, 0, unroll=UNROLL)


def forecast_kernel(field, x_ref, before_ref, after_ref, flux_ref, mask_ref, diff_ref, mix_ref,
                    *rest):
    if field == 0:
        index_ref, out_ref, observed_ref, now, later, crowd, flux, packed, sems, surface = rest
    else:
        _, out_ref, now, later, crowd, flux, packed, sems = rest
    rows, width = x_ref.shape[3], x_ref.shape[4]
    tall = rows + 2 * HALO
    blocks = width // LANES
    level = lax.broadcasted_iota(jnp.int32, (LEVELS, width), 0)

    lateral = jnp.zeros((LEVELS, width), jnp.float32)
    above = jnp.zeros((LEVELS, width), jnp.float32)
    below = jnp.zeros((LEVELS, width), jnp.float32)
    for l in range(LEVELS):
        lateral = jnp.where(level == l, diff_ref[field, l], lateral)
        if l < LEVELS - 1:
            above = jnp.where(level == l, mix_ref[field, l], above)
            below = jnp.where(level == l + 1, mix_ref[field, l], below)
    coef = (lateral, above, below)

    sea = mask_ref[1 : tall - 1, :]
    crowd[1 : tall - 1, :] = (
        mask_ref[0 : tall - 2, :] + mask_ref[2:tall, :]
        + pltpu.roll(sea, 1, 1) + pltpu.roll(sea, width - 1, 1)
    )
    flux[0:1, :] = before_ref[field, HALO * LEVELS : HALO * LEVELS + 1, :]
    flux[1 : rows + 1, :] = flux_ref[0, field]
    flux[rows + 1 : rows + 2, :] = after_ref[field, HALO * LEVELS : HALO * LEVELS + 1, :]
    for h in range(HALO):
        now[h] = before_ref[field, h * LEVELS : (h + 1) * LEVELS, :]
        now[HALO + rows + h] = after_ref[field, h * LEVELS : (h + 1) * LEVELS, :]

    def turn(b, _):
        start = pl.multiple_of(b * 8, 8)
        now[pl.ds(HALO + start, 8)] = jnp.swapaxes(x_ref[0, field, :, pl.ds(start, 8), :], 0, 1)
        return 0

    lax.fori_loop(0, rows // 8, turn, 0)

    def keep(r, value):
        later[r] = value

    stencil_rows(now, keep, 1, tall - 1, field, mask_ref, crowd, flux, coef)

    def emit(r, value):
        row = r - HALO
        tile = row // 2
        side = row % 2
        for j in range(blocks):
            packed[tile, side * blocks + j] = value[:, j * LANES : (j + 1) * LANES]
        if field == 0:
            surface[side, pl.ds(tile, 1), :] = value[0:1, :]

    groups = sems.shape[0]
    share = rows // groups
    copies = []
    for g in range(groups):
        first = HALO + g * share
        stencil_rows(later, emit, first, first + share, field, mask_ref, crowd, flux, coef)
        part = pl.ds(g * share // 2, share // 2)
        copy = pltpu.make_async_copy(
            packed.at[part],
            out_ref.at[part, pl.ds(field * 2 * blocks, 2 * blocks)],
            sems.at[g],
        )
        copy.start()
        copies.append(copy)

    if field == 0:
        tiles = rows // 2
        slots = index_ref.shape[2]
        for g in range(tiles // 8):
            for h in range(slots // LANES):
                where = index_ref[0, g * 8 : (g + 1) * 8, h * LANES : (h + 1) * LANES]
                block, lane = where >> 7, where & (LANES - 1)
                found = jnp.zeros((8, LANES), jnp.float32)
                for q in range(2 * blocks):
                    s, j = divmod(q, blocks)
                    source = surface[s, g * 8 : (g + 1) * 8, j * LANES : (j + 1) * LANES]
                    taken = jnp.take_along_axis(source, lane, axis=1, mode="promise_in_bounds")
                    found = jnp.where(block == q, taken, found)
                observed_ref[g * 8 : (g + 1) * 8, h, :] = found
    for copy in copies:
        copy.wait()


def gram_kernel(tile_ref, seen_ref, value_ref, error_ref, count_ref, _, out_ref, spread, sem):
    tile = tile_ref[0]
    halves = seen_ref.shape[1]
    members = seen_ref.shape[0]
    slot = lax.broadcasted_iota(jnp.int32, (1, LANES), 1)
    total = jnp.zeros((members + 8, members), jnp.float32)
    for h in range(halves):
        seen = seen_ref[:, h, :]
        average = jnp.mean(seen, axis=0, keepdims=True)
        anomaly = seen - average
        span = slice(h * LANES, (h + 1) * LANES)
        own = lax.broadcasted_iota(jnp.int32, (value_ref.shape[1], LANES), 0) == tile
        value = jnp.sum(jnp.where(own, value_ref[0, :, span], 0.0), axis=0, keepdims=True)
        error = jnp.sum(jnp.where(own, error_ref[0, :, span], 0.0), axis=0, keepdims=True)
        active = jnp.where(slot + h * LANES < count_ref[0, tile], 1.0, 0.0)
        weight = active / error
        drift = weight * (value - average)
        left = jnp.concatenate([anomaly * weight, jnp.broadcast_to(drift, (8, LANES))], axis=0)
        total = total + lax.dot_general(
            left, anomaly, (((1,), (1,)), ((), ())),
            precision=lax.Precision.HIGHEST, preferred_element_type=jnp.float32,
        )
    packed = jnp.concatenate([total[g * 8 : (g + 1) * 8] for g in range(4)], axis=1)
    pull = jnp.concatenate([total[members : members + 8]] * 4, axis=1)
    row = lax.broadcasted_iota(jnp.int32, packed.shape, 0)
    lane = lax.broadcasted_iota(jnp.int32, packed.shape, 1)
    corner = (lane >= 16) & (lane < 32)
    packed = jnp.where(corner & (row == 0), pltpu.roll(pull, 16, 1), packed)
    packed = jnp.where(corner & (row == 1), pull, packed)
    spread[...] = jnp.broadcast_to(packed[None, None], spread.shape)
    copy = pltpu.make_async_copy(spread, out_ref.at[:, pl.ds(out_ref.shape[1] - 1, 1)], sem)
    copy.start()
    copy.wait()


def ensemble_kernel(packed, wide):
    count = 32
    lane = lax.broadcasted_iota(jnp.int32, (count, LANES), 1)
    row = lax.broadcasted_iota(jnp.int32, (count, LANES), 0)
    gram = jnp.concatenate(
        [packed if g == 0 else pltpu.roll(packed, LANES - g * count, 1) for g in range(4)], axis=0
    )
    pull = jnp.where(
        lane[0:1] < 16,
        pltpu.roll(packed[0:8], LANES - 16, 1)[0:1],
        packed[1:2],
    )
    gram = gram + jnp.where(lane == row, count - 1.0, 0.0)
    columns = [jnp.broadcast_to(gram[:, k : k + 1], (count, LANES)) for k in range(count)]
    work = jnp.where(lane == row, 1.0, 0.0)
    for k in range(count):
        base = (k // 8) * 8
        column = columns[k][base:]
        pivot = jnp.broadcast_to(column[k - base : k - base + 1], (8, LANES))
        scale = lax.rsqrt(pivot)
        scale = scale * (1.5 - 0.5 * pivot * scale * scale)
        head = scale[0:1]
        lead = work[k : k + 1] * head
        column = column * head
        below = row[base:] > k
        factor = jnp.where(below, column, 0.0)
        rest = jnp.where(row[base:] == k, lead, work[base:] - factor * lead)
        work = rest if base == 0 else jnp.concatenate([work[:base], rest], axis=0)
        for c in range(k + 1, count):
            cbase = (c // 8) * 8
            ratio = column[c - base : c - base + 1]
            old = columns[c]
            fresh = old[cbase:] - column[cbase - base :] * ratio
            columns[c] = fresh if cbase == 0 else jnp.concatenate([old[:cbase], fresh], axis=0)
    inverse = work
    gained = jnp.sum(inverse * pull, axis=1, keepdims=True)
    mean_weight = jnp.sum(inverse * gained, axis=0, keepdims=True)
    live = lane < count
    weights = jnp.where(live, mean_weight + jnp.sqrt(count - 1.0) * inverse, 0.0)
    centre = jnp.sum(weights, axis=1, keepdims=True) * (1.0 / count)
    return jnp.where(live, weights - centre + 1.0 / count, 0.0)


def mix_kernel(data_ref, mask_ref, out_ref, high, low):
    members, slabs = data_ref.shape[0], data_ref.shape[1]
    blocks = mask_ref.shape[1] // LANES
    deep = members * LEVELS

    kernel = ensemble_kernel(jnp.sum(data_ref[:, slabs - 1], axis=0), LANES)[:, :members]
    major = kernel.astype(jnp.bfloat16)
    minor = (kernel - major.astype(jnp.float32)).astype(jnp.bfloat16)
    spread = (
        lax.broadcasted_iota(jnp.int32, (deep, members), 0) // LEVELS
        == lax.broadcasted_iota(jnp.int32, (deep, members), 1)
    ).astype(jnp.bfloat16)
    same = (
        lax.broadcasted_iota(jnp.int32, (deep, deep), 0) % LEVELS
        == lax.broadcasted_iota(jnp.int32, (deep, deep), 1) % LEVELS
    )
    for part, target in ((major, high), (minor, low)):
        tall = jnp.dot(spread, part, preferred_element_type=jnp.float32).astype(jnp.bfloat16)
        full = lax.dot_general(
            tall, spread, (((1,), (1,)), ((), ())), preferred_element_type=jnp.float32
        )
        target[...] = jnp.where(same, full, 0.0).astype(jnp.bfloat16)

    def strip(i, _):
        first = i * blocks
        data = jnp.concatenate(
            [data_ref[:, first + b].reshape(deep, LANES) for b in range(blocks)], axis=1
        )
        major = data.astype(jnp.bfloat16)
        minor = (data - major.astype(jnp.float32)).astype(jnp.bfloat16)
        mixed = jnp.dot(high[...], major, preferred_element_type=jnp.float32)
        mixed = mixed + jnp.dot(high[...], minor, preferred_element_type=jnp.float32)
        mixed = mixed + jnp.dot(low[...], major, preferred_element_type=jnp.float32)
        ocean = mask_ref[pl.ds(i % 2, 1), :] > 0.0
        mixed = jnp.where(ocean, mixed, data)
        for b in range(blocks):
            out_ref[:, first + b] = mixed[:, b * LANES : (b + 1) * LANES].reshape(
                members, LEVELS, LANES
            )
        return 0

    lax.fori_loop(0, FIELDS * 2, strip, 0)


def settle_kernel(back_ref, out_ref):
    blocks = out_ref.shape[4] // LANES
    share = out_ref.shape[3] // 2
    first = pl.program_id(0) * share
    for f in range(FIELDS):
        for j in range(blocks):
            for half in range(share // 4):
                rows = []
                for t in range(4):
                    for s in range(2):
                        rows.append(back_ref[first + half * 4 + t, (f * 2 + s) * blocks + j])
                turned = jnp.swapaxes(jnp.stack(rows, axis=0), 0, 1)
                out_ref[0, f, :, half * 8 : (half + 1) * 8, j * LANES : (j + 1) * LANES] = turned


def shards(
    starting_tracer_fields,
    surface_exchange_inputs,
    diffusivity,
    mixing,
    land_mask,
    obs_index,
    obs_count,
    obs_value,
    obs_error,
):
    _, fields, levels, rows, width = starting_tracer_fields.shape
    members = lax.axis_size("member")
    domains = lax.axis_size("domain")
    blocks = width // LANES
    tiles = members
    per_field = 2 * blocks
    slabs = fields * per_field + 1
    tile = lax.axis_index("member")
    domain = lax.axis_index("domain")
    state, flux = starting_tracer_fields[0], surface_exchange_inputs[0]

    def edge(first, flux_row):
        lines = jnp.swapaxes(state[:, :, first : first + HALO], 1, 2)
        lines = lines.reshape(fields, HALO * levels, width)
        return jnp.concatenate([lines, flux[:, flux_row : flux_row + 1]], axis=1)

    up = [(i, i + 1) for i in range(domains - 1)]
    down = [(i + 1, i) for i in range(domains - 1)]
    before = lax.ppermute(edge(rows - HALO, rows - 1), "domain", up)
    after = lax.ppermute(edge(0, 0), "domain", down)

    padded = jnp.pad(land_mask, ((HALO, HALO), (0, 0)))
    mask = lax.dynamic_slice_in_dim(padded, domain * rows, rows + 2 * HALO, 0).astype(jnp.float32)
    tile_mask = lax.dynamic_slice_in_dim(mask, HALO + tile * 2, 2, 0)

    f32 = jnp.float32
    tall = rows + 2 * HALO
    bulk = jax.ShapeDtypeStruct((tiles, slabs, levels, LANES), f32)

    vmem = pl.BlockSpec(memory_space=pltpu.VMEM)
    smem = pl.BlockSpec(memory_space=pltpu.SMEM)
    anywhere = pl.BlockSpec(memory_space=pl.ANY)

    def forecast(field, extra):
        in_specs = [vmem] * 5 + [smem] * 2
        out_shape = [bulk]
        out_specs = [anywhere]
        scratch = [
            pltpu.VMEM((tall, levels, width), f32),
            pltpu.VMEM((tall, levels, width), f32),
            pltpu.VMEM((tall, width), f32),
            pltpu.VMEM((rows + 2, width), f32),
            pltpu.VMEM((tiles, per_field, levels, LANES), f32),
            pltpu.SemaphoreType.DMA((4,)),
        ]
        alias = {}
        if field == 0:
            in_specs.append(vmem)
            slots = obs_index.shape[2]
            out_shape.append(jax.ShapeDtypeStruct((tiles, slots // LANES, LANES), f32))
            out_specs.append(vmem)
            scratch.append(pltpu.VMEM((2, tiles, width), f32))
        else:
            in_specs.append(anywhere)
            alias = {7: 0}
        return pl.pallas_call(
            functools.partial(forecast_kernel, field),
            out_shape=out_shape,
            in_specs=in_specs,
            out_specs=out_specs,
            scratch_shapes=scratch,
            input_output_aliases=alias,
            compiler_params=pltpu.CompilerParams(vmem_limit_bytes=16 << 20),
            cost_estimate=pl.CostEstimate(
                flops=40_000_000, bytes_accessed=3_000_000, transcendentals=0
            ),
            name=f"forecast_{field}",
        )(
            starting_tracer_fields, before, after, surface_exchange_inputs, mask,
            diffusivity, mixing, extra,
        )

    sent, observed = forecast(0, obs_index)
    seen = lax.all_to_all(observed, "member", split_axis=0, concat_axis=0, tiled=True)
    (sent,) = forecast(1, sent)

    sent = pl.pallas_call(
        gram_kernel,
        out_shape=bulk,
        in_specs=[smem, vmem, vmem, vmem, smem, anywhere],
        out_specs=anywhere,
        scratch_shapes=[
            pltpu.VMEM((tiles, 1, levels, LANES), f32),
            pltpu.SemaphoreType.DMA,
        ],
        input_output_aliases={5: 0},
        compiler_params=pltpu.CompilerParams(vmem_limit_bytes=8 << 20),
        name="gram",
    )(tile.reshape(1).astype(jnp.int32), seen, obs_value, obs_error, obs_count, sent)

    held = lax.all_to_all(sent, "member", split_axis=0, concat_axis=0, tiled=True)

    deep = members * levels
    updated = pl.pallas_call(
        mix_kernel,
        out_shape=jax.ShapeDtypeStruct((members, slabs - 1, levels, LANES), f32),
        in_specs=[vmem, vmem],
        out_specs=vmem,
        scratch_shapes=[
            pltpu.VMEM((deep, deep), jnp.bfloat16),
            pltpu.VMEM((deep, deep), jnp.bfloat16),
        ],
        compiler_params=pltpu.CompilerParams(vmem_limit_bytes=16 << 20),
        name="mix",
    )(held, tile_mask)

    back = lax.all_to_all(updated, "member", split_axis=0, concat_axis=0, tiled=True)

    return pl.pallas_call(
        settle_kernel,
        grid=(rows // 16,),
        out_shape=jax.ShapeDtypeStruct(starting_tracer_fields.shape, f32),
        in_specs=[vmem],
        out_specs=pl.BlockSpec((1, fields, levels, 16, width), lambda i: (0, 0, 0, i, 0)),
        compiler_params=pltpu.CompilerParams(vmem_limit_bytes=16 << 20),
        name="settle",
    )(back)


def solution(mesh):
    placed = (
        P("member", None, None, "domain", None),
        P("member", None, "domain", None),
        P(),
        P(),
        P(),
        P("domain", None, None),
        P("domain", None),
        P("domain", None, None),
        P("domain", None, None),
    )
    return jax.shard_map(
        shards,
        mesh=mesh,
        in_specs=placed,
        out_specs=P("member", None, None, "domain", None),
        check_vma=False,
    )
```

```python
import functools

import jax
import jax.numpy as jnp
from jax import lax
from jax.experimental import pallas as pl
from jax.experimental.pallas import tpu as pltpu
from jax.sharding import PartitionSpec as P

FIELDS = 2
LEVELS = 8
LANES = 128
HALO = 2
UNROLL = 10


def spread_row(row):
    return jnp.broadcast_to(row, (LEVELS, row.shape[1]))


def prepare_kernel(field, x_ref, flux_ref, mask_ref, *rest):
    turned, wet, source, sea8, crowd8, held, sems = rest[-7:]
    rows, width = turned.shape[0], turned.shape[2]
    tall = rows + 2 * HALO
    parts = rows // 8
    copies = []
    for p in range(parts):
        span = pl.ds(p * 8, 8)
        copy = pltpu.make_async_copy(
            x_ref.at[0, field, :, span, :], held.at[:, span, :], sems.at[p]
        )
        copy.start()
        copies.append(copy)
    sea = mask_ref[1 : tall - 1, :]
    crowd = (
        mask_ref[0 : tall - 2, :] + mask_ref[2:tall, :]
        + pltpu.roll(sea, 1, 1) + pltpu.roll(sea, width - 1, 1)
    )
    for r in range(tall):
        sea8[r] = spread_row(mask_ref[r : r + 1, :])
    for r in range(1, tall - 1):
        crowd8[r] = spread_row(crowd[r - 1 : r, :])
    top = lax.broadcasted_iota(jnp.int32, (LEVELS, width), 0) == 0
    for p in range(parts):
        copies[p].wait()
        start = p * 8
        flipped = jnp.swapaxes(held[:, start : start + 8, :], 0, 1)
        for k in range(8):
            r = start + k
            turned[r] = flipped[k]
            wet[r] = flipped[k] * sea8[r + HALO]
            source[r] = jnp.where(top, spread_row(flux_ref[0, field, r : r + 1, :]), 0.0)


def forecast_kernel(field, turned, wet, source, sea8, crowd8, before_ref, after_ref,
                    diff_ref, mix_ref, *rest):
    if field == 0:
        index_ref, out_ref, done_ref, first, moist, packed, sems, surface = rest
        done_ref[...] = jnp.zeros_like(done_ref)
    else:
        out_ref, first, moist, packed, sems = rest
    rows, width = turned.shape[0], turned.shape[2]
    tall = rows + 2 * HALO
    blocks = width // LANES

    level = lax.broadcasted_iota(jnp.int32, (LEVELS, LEVELS), 0)
    lane = lax.broadcasted_iota(jnp.int32, (LEVELS, LEVELS), 1)
    diff = diff_ref[field : field + 1, :]
    mix = jnp.concatenate([mix_ref[field : field + 1, :], jnp.zeros((1, 1), jnp.float32)], axis=1)

    def along(table, shift):
        column = jnp.sum(jnp.where(lane + shift == level, table, 0.0), axis=1, keepdims=True)
        return jnp.concatenate([jnp.broadcast_to(column, (LEVELS, LANES))] * blocks, axis=1)

    lateral, above, below = along(diff, 0), along(mix, 0), along(mix, 1)
    vertical = above + below

    def stepped(r, x, y, north, south, gain):
        sea = sea8[r]
        around = north + south + pltpu.roll(y, 1, 1) + pltpu.roll(y, width - 1, 1)
        change = lateral * (around - crowd8[r] * x) - vertical * x + gain
        change = change + above * pltpu.roll(x, LEVELS - 1, 0)
        change = change + below * pltpu.roll(x, 1, 0)
        return x + sea * change

    def near(r):
        if r < HALO:
            x = before_ref[field, r * LEVELS : (r + 1) * LEVELS, :]
        elif r >= HALO + rows:
            h = r - HALO - rows
            x = after_ref[field, h * LEVELS : (h + 1) * LEVELS, :]
        else:
            return turned[r - HALO], wet[r - HALO]
        return x, x * sea8[r]

    top = lax.broadcasted_iota(jnp.int32, (LEVELS, width), 0) == 0

    def gain_at(r):
        if HALO <= r < HALO + rows:
            return source[r - HALO]
        ref = before_ref if r < HALO else after_ref
        line = ref[field, HALO * LEVELS : HALO * LEVELS + 1, :]
        return jnp.where(top, spread_row(line), 0.0)

    def keep(r, value):
        first[r] = value
        moist[r] = value * sea8[r]

    def inner(r, _):
        i = r - HALO
        keep(r, stepped(r, turned[i], wet[i], wet[i - 1], wet[i + 1], source[i]))
        return 0

    body = (tall - 6) // UNROLL * UNROLL
    for r in (1, 2, *range(3 + body, tall - 1)):
        x, y = near(r)
        keep(r, stepped(r, x, y, near(r - 1)[1], near(r + 1)[1], gain_at(r)))
    lax.fori_loop(3, 3 + body, inner, 0, unroll=UNROLL)

    def outer(tile, _):
        for side in range(2):
            r = HALO + 2 * tile + side
            value = stepped(r, first[r], moist[r], moist[r - 1], moist[r + 1], source[r - HALO])
            for j in range(blocks):
                packed[tile, side * blocks + j] = value[:, j * LANES : (j + 1) * LANES]
            if field == 0:
                surface[side, pl.ds(tile, 1), :] = value[0:1, :]
        return 0

    tiles = rows // 2
    groups = 4
    share = tiles // groups
    copies = []
    for g in range(groups):
        lax.fori_loop(g * share, (g + 1) * share, outer, 0, unroll=4)
        part = (pl.ds(g * share, share), pl.ds(0, 2 * blocks))
        copies.append(pltpu.make_async_copy(packed.at[part], out_ref.at[part], sems.at[g]))
        copies[-1].start()

    if field == 0:
        slots = index_ref.shape[2]
        for g in range(tiles // 8):
            for h in range(slots // LANES):
                where = index_ref[0, g * 8 : (g + 1) * 8, h * LANES : (h + 1) * LANES]
                block, lanes = where >> 7, where & (LANES - 1)
                found = jnp.zeros((8, LANES), jnp.float32)
                for q in range(2 * blocks):
                    s, j = divmod(q, blocks)
                    piece = surface[s, g * 8 : (g + 1) * 8, j * LANES : (j + 1) * LANES]
                    taken = jnp.take_along_axis(piece, lanes, axis=1, mode="promise_in_bounds")
                    found = jnp.where(block == q, taken, found)
                packed[g * 8 : (g + 1) * 8, 2 * blocks, h, :] = found
        part = (slice(None), pl.ds(2 * blocks, 1))
        copies.append(pltpu.make_async_copy(packed.at[part], out_ref.at[part], sems.at[groups]))
        copies[-1].start()
    for copy in copies:
        copy.wait()


def gram_kernel(tile_ref, held_ref, value_ref, error_ref, count_ref, _, out_ref, spread, sem):
    tile = tile_ref[0]
    members, per_field = held_ref.shape[0], held_ref.shape[1] - 1
    halves = value_ref.shape[2] // LANES
    slot = lax.broadcasted_iota(jnp.int32, (1, LANES), 1)
    total = jnp.zeros((members + 8, members), jnp.float32)
    for h in range(halves):
        seen = held_ref[:, per_field, h, :]
        average = jnp.mean(seen, axis=0, keepdims=True)
        anomaly = seen - average
        span = slice(h * LANES, (h + 1) * LANES)
        own = lax.broadcasted_iota(jnp.int32, (value_ref.shape[1], LANES), 0) == tile
        value = jnp.sum(jnp.where(own, value_ref[0, :, span], 0.0), axis=0, keepdims=True)
        error = jnp.sum(jnp.where(own, error_ref[0, :, span], 0.0), axis=0, keepdims=True)
        active = jnp.where(slot + h * LANES < count_ref[0, tile], 1.0, 0.0)
        weight = active / error
        drift = weight * (value - average)
        left = jnp.concatenate([anomaly * weight, jnp.broadcast_to(drift, (8, LANES))], axis=0)
        total = total + lax.dot_general(
            left, anomaly, (((1,), (1,)), ((), ())),
            precision=lax.Precision.HIGHEST, preferred_element_type=jnp.float32,
        )
    packed = jnp.concatenate([total[g * 8 : (g + 1) * 8] for g in range(4)], axis=1)
    pull = jnp.concatenate([total[members : members + 8]] * 4, axis=1)
    row = lax.broadcasted_iota(jnp.int32, packed.shape, 0)
    lane = lax.broadcasted_iota(jnp.int32, packed.shape, 1)
    corner = (lane >= 16) & (lane < 32)
    packed = jnp.where(corner & (row == 0), pltpu.roll(pull, 16, 1), packed)
    packed = jnp.where(corner & (row == 1), pull, packed)
    for m in range(members):
        spread[m, 0] = packed
    copy = pltpu.make_async_copy(spread, out_ref.at[:, pl.ds(per_field, 1)], sem)
    copy.start()
    copy.wait()


def ensemble_kernel(packed, wide):
    count = 32
    lane = lax.broadcasted_iota(jnp.int32, (count, LANES), 1)
    row = lax.broadcasted_iota(jnp.int32, (count, LANES), 0)
    gram = jnp.concatenate(
        [packed if g == 0 else pltpu.roll(packed, LANES - g * count, 1) for g in range(4)], axis=0
    )
    pull = jnp.where(
        lane[0:1] < 16,
        pltpu.roll(packed[0:8], LANES - 16, 1)[0:1],
        packed[1:2],
    )
    gram = gram + jnp.where(lane == row, count - 1.0, 0.0)
    columns = [jnp.broadcast_to(gram[:, k : k + 1], (count, LANES)) for k in range(count)]
    work = jnp.where(lane == row, 1.0, 0.0)
    for k in range(count):
        base = (k // 8) * 8
        column = columns[k][base:]
        pivot = jnp.broadcast_to(column[k - base : k - base + 1], (8, LANES))
        scale = lax.rsqrt(pivot)
        scale = scale * (1.5 - 0.5 * pivot * scale * scale)
        head = scale[0:1]
        lead = work[k : k + 1] * head
        column = column * head
        below = row[base:] > k
        factor = jnp.where(below, column, 0.0)
        rest = jnp.where(row[base:] == k, lead, work[base:] - factor * lead)
        work = rest if base == 0 else jnp.concatenate([work[:base], rest], axis=0)
        for c in range(k + 1, count):
            cbase = (c // 8) * 8
            ratio = column[c - base : c - base + 1]
            old = columns[c]
            fresh = old[cbase:] - column[cbase - base :] * ratio
            columns[c] = fresh if cbase == 0 else jnp.concatenate([old[:cbase], fresh], axis=0)
    inverse = work
    gained = jnp.sum(inverse * pull, axis=1, keepdims=True)
    mean_weight = jnp.sum(inverse * gained, axis=0, keepdims=True)
    live = lane < count
    weights = jnp.where(live, mean_weight + jnp.sqrt(count - 1.0) * inverse, 0.0)
    centre = jnp.sum(weights, axis=1, keepdims=True) * (1.0 / count)
    return jnp.where(live, weights - centre + 1.0 / count, 0.0)


def mix_kernel(data0_ref, data1_ref, mask_ref, out_ref, high, low):
    members, per_field = data0_ref.shape[0], data0_ref.shape[1] - 1
    blocks = mask_ref.shape[1] // LANES
    deep = members * LEVELS

    kernel = ensemble_kernel(jnp.sum(data1_ref[:, per_field], axis=0), LANES)[:, :members]
    major = kernel.astype(jnp.bfloat16)
    minor = (kernel - major.astype(jnp.float32)).astype(jnp.bfloat16)
    spread = (
        lax.broadcasted_iota(jnp.int32, (deep, members), 0) // LEVELS
        == lax.broadcasted_iota(jnp.int32, (deep, members), 1)
    ).astype(jnp.bfloat16)
    same = (
        lax.broadcasted_iota(jnp.int32, (deep, deep), 0) % LEVELS
        == lax.broadcasted_iota(jnp.int32, (deep, deep), 1) % LEVELS
    )
    for part, target in ((major, high), (minor, low)):
        tall = jnp.dot(spread, part, preferred_element_type=jnp.float32).astype(jnp.bfloat16)
        full = lax.dot_general(
            tall, spread, (((1,), (1,)), ((), ())), preferred_element_type=jnp.float32
        )
        target[...] = jnp.where(same, full, 0.0).astype(jnp.bfloat16)

    for f, data_ref in ((0, data0_ref), (1, data1_ref)):

        def strip(i, _, f=f, data_ref=data_ref):
            first = i * blocks
            data = jnp.concatenate(
                [data_ref[:, first + b].reshape(deep, LANES) for b in range(blocks)], axis=1
            )
            major = data.astype(jnp.bfloat16)
            minor = (data - major.astype(jnp.float32)).astype(jnp.bfloat16)
            mixed = jnp.dot(high[...], major, preferred_element_type=jnp.float32)
            mixed = mixed + jnp.dot(high[...], minor, preferred_element_type=jnp.float32)
            mixed = mixed + jnp.dot(low[...], major, preferred_element_type=jnp.float32)
            ocean = mask_ref[pl.ds(i, 1), :] > 0.0
            mixed = jnp.where(ocean, mixed, data)
            for b in range(blocks):
                out_ref[:, f * per_field + first + b] = mixed[
                    :, b * LANES : (b + 1) * LANES
                ].reshape(members, LEVELS, LANES)
            return 0

        lax.fori_loop(0, 2, strip, 0)


def settle_kernel(back_ref, out_ref):
    blocks = out_ref.shape[4] // LANES
    share = out_ref.shape[3] // 2
    first = pl.program_id(0) * share
    for f in range(FIELDS):
        for j in range(blocks):
            for half in range(share // 4):
                rows = []
                for t in range(4):
                    for s in range(2):
                        rows.append(back_ref[first + half * 4 + t, (f * 2 + s) * blocks + j])
                turned = jnp.swapaxes(jnp.stack(rows, axis=0), 0, 1)
                out_ref[0, f, :, half * 8 : (half + 1) * 8, j * LANES : (j + 1) * LANES] = turned


def shards(
    starting_tracer_fields,
    surface_exchange_inputs,
    diffusivity,
    mixing,
    land_mask,
    obs_index,
    obs_count,
    obs_value,
    obs_error,
):
    _, fields, levels, rows, width = starting_tracer_fields.shape
    members = lax.axis_size("member")
    domains = lax.axis_size("domain")
    blocks = width // LANES
    tiles = members
    per_field = 2 * blocks
    tile = lax.axis_index("member")
    domain = lax.axis_index("domain")
    state, flux = starting_tracer_fields[0], surface_exchange_inputs[0]

    def edge(first, flux_row):
        lines = jnp.swapaxes(state[:, :, first : first + HALO], 1, 2)
        lines = lines.reshape(fields, HALO * levels, width)
        return jnp.concatenate([lines, flux[:, flux_row : flux_row + 1]], axis=1)

    up = [(i, i + 1) for i in range(domains - 1)]
    down = [(i + 1, i) for i in range(domains - 1)]
    before = lax.ppermute(edge(rows - HALO, rows - 1), "domain", up)
    after = lax.ppermute(edge(0, 0), "domain", down)

    padded = jnp.pad(land_mask, ((HALO, HALO), (0, 0)))
    mask = lax.dynamic_slice_in_dim(padded, domain * rows, rows + 2 * HALO, 0).astype(jnp.float32)
    tile_mask = lax.dynamic_slice_in_dim(mask, HALO + tile * 2, 2, 0)

    f32 = jnp.float32
    tall = rows + 2 * HALO
    vmem = pl.BlockSpec(memory_space=pltpu.VMEM)
    smem = pl.BlockSpec(memory_space=pltpu.SMEM)
    anywhere = pl.BlockSpec(memory_space=pl.ANY)
    hbm = pl.BlockSpec(memory_space=pltpu.HBM)

    def params(mib):
        return pltpu.CompilerParams(vmem_limit_bytes=mib << 20)

    band = jax.ShapeDtypeStruct((rows, levels, width), f32)
    shell = jax.ShapeDtypeStruct((tall, levels, width), f32)
    bulk = jax.ShapeDtypeStruct((tiles, per_field + 1, levels, LANES), f32)
    mark = jax.ShapeDtypeStruct((levels, LANES), f32)

    def prepare(field, *after_this):
        return pl.pallas_call(
            functools.partial(prepare_kernel, field),
            out_shape=[band, band, band, shell, shell],
            in_specs=[hbm, vmem, vmem] + [anywhere] * len(after_this),
            out_specs=[vmem] * 5,
            scratch_shapes=[
                pltpu.VMEM((levels, rows, width), f32),
                pltpu.SemaphoreType.DMA((rows // 8,)),
            ],
            compiler_params=params(8),
            cost_estimate=pl.CostEstimate(
                flops=20_000_000, bytes_accessed=3_000_000, transcendentals=0
            ),
            name=f"prepare_{field}",
        )(
            pltpu.with_memory_space_constraint(starting_tracer_fields, pltpu.HBM),
            surface_exchange_inputs, mask, *after_this,
        )

    def forecast(field, prepared, *extra):
        scratch = [
            pltpu.VMEM((tall, levels, width), f32),
            pltpu.VMEM((tall, levels, width), f32),
            pltpu.VMEM(bulk.shape, f32),
            pltpu.SemaphoreType.DMA((5,)),
        ]
        if field == 0:
            scratch.append(pltpu.VMEM((2, tiles, width), f32))
        return pl.pallas_call(
            functools.partial(forecast_kernel, field),
            out_shape=[bulk, mark] if field == 0 else bulk,
            in_specs=[vmem] * (9 + len(extra)),
            out_specs=[anywhere, vmem] if field == 0 else anywhere,
            scratch_shapes=scratch,
            compiler_params=params(8),
            cost_estimate=pl.CostEstimate(
                flops=40_000_000, bytes_accessed=3_000_000, transcendentals=0
            ),
            name=f"forecast_{field}",
        )(*prepared, before, after, diffusivity, mixing, *extra)

    sent0, done0 = forecast(0, prepare(0), obs_index)
    held0 = lax.all_to_all(sent0, "member", split_axis=0, concat_axis=0, tiled=True)
    sent1 = forecast(1, prepare(1, done0))
    sent1 = pl.pallas_call(
        gram_kernel,
        out_shape=bulk,
        in_specs=[smem, vmem, vmem, vmem, smem, anywhere],
        out_specs=anywhere,
        scratch_shapes=[
            pltpu.VMEM((tiles, 1, levels, LANES), f32),
            pltpu.SemaphoreType.DMA,
        ],
        input_output_aliases={5: 0},
        compiler_params=params(4),
        name="gram",
    )(tile.reshape(1).astype(jnp.int32), held0, obs_value, obs_error, obs_count, sent1)
    held1 = lax.all_to_all(sent1, "member", split_axis=0, concat_axis=0, tiled=True)

    deep = members * levels
    updated = pl.pallas_call(
        mix_kernel,
        out_shape=jax.ShapeDtypeStruct((members, fields * per_field, levels, LANES), f32),
        in_specs=[vmem, vmem, vmem],
        out_specs=vmem,
        scratch_shapes=[
            pltpu.VMEM((deep, deep), jnp.bfloat16),
            pltpu.VMEM((deep, deep), jnp.bfloat16),
        ],
        compiler_params=params(16),
        name="mix",
    )(held0, held1, tile_mask)

    back = lax.all_to_all(updated, "member", split_axis=0, concat_axis=0, tiled=True)

    return pl.pallas_call(
        settle_kernel,
        grid=(rows // 16,),
        out_shape=jax.ShapeDtypeStruct(starting_tracer_fields.shape, f32),
        in_specs=[vmem],
        out_specs=pl.BlockSpec((1, fields, levels, 16, width), lambda i: (0, 0, 0, i, 0)),
        compiler_params=params(16),
        name="settle",
    )(back)


def solution(mesh):
    placed = (
        P("member", None, None, "domain", None),
        P("member", None, "domain", None),
        P(),
        P(),
        P(),
        P("domain", None, None),
        P("domain", None),
        P("domain", None, None),
        P("domain", None, None),
    )
    return jax.shard_map(
        shards,
        mesh=mesh,
        in_specs=placed,
        out_specs=P("member", None, None, "domain", None),
        check_vma=False,
    )
```

```python
import functools

import jax
import jax.numpy as jnp
from jax import lax
from jax.experimental import pallas as pl
from jax.experimental.pallas import tpu as pltpu
from jax.sharding import PartitionSpec as P

FIELDS = 2
LEVELS = 8
LANES = 128
HALO = 2
UNROLL = 10
PACKED = 9
TAIL = 32
ROOM = PACKED * LANES - TAIL
SPILL = 2


def spread_row(row):
    return jnp.broadcast_to(row, (LEVELS, row.shape[1]))


def survey_kernel(mask_ref, cell_ref, place_ref, first_ref, head_ref, sea_ref):
    tiles, cells = place_ref.shape
    rows = 2 * tiles
    blocks = cells // LANES
    sea_ref[...] = mask_ref[HALO : HALO + rows, :]
    sea = mask_ref[HALO : HALO + rows, :].astype(jnp.bfloat16)
    pick = lax.broadcasted_iota(jnp.int32, (tiles, rows), 1) - 2 * lax.broadcasted_iota(
        jnp.int32, (tiles, rows), 0
    )
    sides = [
        jnp.dot((pick == s).astype(jnp.bfloat16), sea, preferred_element_type=jnp.float32)
        for s in range(2)
    ]
    sea = jnp.concatenate(sides, axis=1)
    land = (1.0 - sea).astype(jnp.bfloat16)
    stacked = jnp.concatenate([land[:, b * LANES : (b + 1) * LANES] for b in range(blocks)], axis=0)
    before = (
        lax.broadcasted_iota(jnp.int32, (LANES, LANES), 0)
        < lax.broadcasted_iota(jnp.int32, (LANES, LANES), 1)
    ).astype(jnp.bfloat16)
    within = jnp.dot(stacked, before, preferred_element_type=jnp.float32)
    totals = jnp.dot(
        stacked, jnp.ones((LANES, LANES), jnp.bfloat16), preferred_element_type=jnp.float32
    )
    offset = jnp.zeros((tiles, LANES), jnp.float32)
    shifts = []
    for b in range(blocks):
        part = slice(b * tiles, (b + 1) * tiles)
        shifts.append(within[part] + offset)
        offset = offset + totals[part]
    shift = jnp.concatenate(shifts, axis=1).astype(jnp.int32)
    cell = lax.broadcasted_iota(jnp.int32, (tiles, cells), 1)
    rank = cell - shift
    place = jnp.where(rank < ROOM, rank, rank + TAIL)
    place_ref[...] = jnp.where(sea > 0.0, place, -1)
    lane = lax.broadcasted_iota(jnp.int32, first_ref.shape, 1)
    first = jnp.zeros(first_ref.shape, jnp.int32)
    for b in range(blocks):
        head = place[:, b * LANES : b * LANES + 1]
        head = (jnp.minimum(head >> 7, PACKED - 1) << 7) + (head & (LANES - 1))
        first = jnp.where(lane == b, jnp.broadcast_to(head, first.shape), first)
    number = lax.broadcasted_iota(jnp.int32, first.shape, 0)
    first = first + number * (FIELDS * PACKED * LANES)
    last = jnp.max(jnp.where(sea > 0.0, place, -1), axis=1, keepdims=True)
    last = jnp.broadcast_to(jnp.max(last, axis=0, keepdims=True), first.shape)
    spills = (last >= PACKED * LANES).astype(jnp.int32)
    first_ref[...] = jnp.where(lane == LANES - 1, spills, first)
    state = jnp.where(sea > 0.0, shift * 2048 + cell, 0)
    for bit in range(11):
        other = pltpu.roll(state, cells - (1 << bit), 1)
        comes = (other & (2048 << bit)) != 0
        goes = (state & (2048 << bit)) != 0
        state = jnp.where(comes, other, jnp.where(goes, 0, state))
    state = state & 2047
    heads = jnp.zeros(head_ref.shape, jnp.int32)
    reach = jnp.zeros((tiles, 1), jnp.int32)
    for q in range(PACKED):
        part = state[:, q * LANES : (q + 1) * LANES]
        heads = jnp.where(lane == q, jnp.broadcast_to(part[:, 0:1], heads.shape), heads)
        reach = jnp.maximum(reach, jnp.max(part, axis=1, keepdims=True) - part[:, 0:1])
    wide = jnp.max(reach, axis=0, keepdims=True)
    heads = heads + number * cells
    heads = jnp.where(lane == PACKED, jnp.broadcast_to(wide, heads.shape), heads)
    head_ref[...] = jnp.where(lane == PACKED + 1, spills, heads)
    state = state + lax.broadcasted_iota(jnp.int32, state.shape, 0) * cells
    cell_ref[:, : PACKED * LANES] = state[:, : PACKED * LANES]
    cell_ref[:, PACKED * LANES :] = pltpu.roll(state, cells - ROOM, 1)[:, : SPILL * LANES]


def prepare_kernel(field, x_ref, flux_ref, mask_ref, *rest):
    turned, wet, source, sea8, crowd8, held, sems = rest[-7:]
    rows, width = turned.shape[0], turned.shape[2]
    tall = rows + 2 * HALO
    parts = rows // 8
    copies = []
    for p in range(parts):
        span = pl.ds(p * 8, 8)
        copy = pltpu.make_async_copy(
            x_ref.at[0, field, :, span, :], held.at[:, span, :], sems.at[p]
        )
        copy.start()
        copies.append(copy)
    sea = mask_ref[1 : tall - 1, :]
    crowd = (
        mask_ref[0 : tall - 2, :] + mask_ref[2:tall, :]
        + pltpu.roll(sea, 1, 1) + pltpu.roll(sea, width - 1, 1)
    )
    for r in range(tall):
        sea8[r] = spread_row(mask_ref[r : r + 1, :])
    for r in range(1, tall - 1):
        crowd8[r] = spread_row(crowd[r - 1 : r, :])
    top = lax.broadcasted_iota(jnp.int32, (LEVELS, width), 0) == 0
    for p in range(parts):
        copies[p].wait()
        start = p * 8
        flipped = jnp.swapaxes(held[:, start : start + 8, :], 0, 1)
        for k in range(8):
            r = start + k
            turned[r] = flipped[k]
            wet[r] = flipped[k] * sea8[r + HALO]
            source[r] = jnp.where(top, spread_row(flux_ref[0, field, r : r + 1, :]), 0.0)


def forecast_kernel(field, turned, wet, source, sea8, crowd8, before_ref, after_ref,
                    diff_ref, mix_ref, *rest):
    cell_ref, head_ref, rest = rest[0], rest[1], rest[2:]
    if field == 0:
        index_ref, out_ref, spill_ref, done_ref, first, moist, plain, packed, heads, sems, surface, tails = rest
        done_ref[...] = jnp.zeros_like(done_ref)
    else:
        out_ref, spill_ref, first, moist, plain, packed, heads, sems = rest
    table = pltpu.make_async_copy(head_ref, heads, sems.at[0])
    table.start()
    rows, width = turned.shape[0], turned.shape[2]
    tall = rows + 2 * HALO
    blocks = width // LANES

    level = lax.broadcasted_iota(jnp.int32, (LEVELS, LEVELS), 0)
    lane = lax.broadcasted_iota(jnp.int32, (LEVELS, LEVELS), 1)
    diff = diff_ref[field : field + 1, :]
    mix = jnp.concatenate([mix_ref[field : field + 1, :], jnp.zeros((1, 1), jnp.float32)], axis=1)

    def along(table, shift):
        column = jnp.sum(jnp.where(lane + shift == level, table, 0.0), axis=1, keepdims=True)
        return jnp.concatenate([jnp.broadcast_to(column, (LEVELS, LANES))] * blocks, axis=1)

    lateral, above, below = along(diff, 0), along(mix, 0), along(mix, 1)
    vertical = above + below

    def stepped(r, x, y, north, south, gain):
        sea = sea8[r]
        around = north + south + pltpu.roll(y, 1, 1) + pltpu.roll(y, width - 1, 1)
        change = lateral * (around - crowd8[r] * x) - vertical * x + gain
        change = change + above * pltpu.roll(x, LEVELS - 1, 0)
        change = change + below * pltpu.roll(x, 1, 0)
        return x + sea * change

    def near(r):
        if r < HALO:
            x = before_ref[field, r * LEVELS : (r + 1) * LEVELS, :]
        elif r >= HALO + rows:
            h = r - HALO - rows
            x = after_ref[field, h * LEVELS : (h + 1) * LEVELS, :]
        else:
            return turned[r - HALO], wet[r - HALO]
        return x, x * sea8[r]

    top = lax.broadcasted_iota(jnp.int32, (LEVELS, width), 0) == 0

    def gain_at(r):
        if HALO <= r < HALO + rows:
            return source[r - HALO]
        ref = before_ref if r < HALO else after_ref
        line = ref[field, HALO * LEVELS : HALO * LEVELS + 1, :]
        return jnp.where(top, spread_row(line), 0.0)

    def keep(r, value):
        first[r] = value
        moist[r] = value * sea8[r]

    def inner(r, _):
        i = r - HALO
        keep(r, stepped(r, turned[i], wet[i], wet[i - 1], wet[i + 1], source[i]))
        return 0

    body = (tall - 6) // UNROLL * UNROLL
    for r in (1, 2, *range(3 + body, tall - 1)):
        x, y = near(r)
        keep(r, stepped(r, x, y, near(r - 1)[1], near(r + 1)[1], gain_at(r)))
    lax.fori_loop(3, 3 + body, inner, 0, unroll=UNROLL)

    def outer(tile, _):
        for side in range(2):
            r = HALO + 2 * tile + side
            value = stepped(r, first[r], moist[r], moist[r - 1], moist[r + 1], source[r - HALO])
            for j in range(blocks):
                plain[tile * 2 * blocks + side * blocks + j] = value[:, j * LANES : (j + 1) * LANES]
            if field == 0:
                surface[side, pl.ds(tile, 1), :] = value[0:1, :]
        return 0

    tiles = rows // 2
    lax.fori_loop(0, tiles, outer, 0, unroll=4)
    table.wait()
    lane_row = lax.broadcasted_iota(jnp.int32, (LEVELS, LANES), 1)

    def take(piece, lanes):
        return jnp.take_along_axis(piece, lanes, axis=1, mode="promise_in_bounds")

    if field == 0:
        slots = index_ref.shape[2]
        for g in range(tiles // 8):
            pieces = []
            for h in range(slots // LANES):
                where = index_ref[0, g * 8 : (g + 1) * 8, h * LANES : (h + 1) * LANES]
                block, lanes = where >> 7, where & (LANES - 1)
                found = jnp.zeros((8, LANES), jnp.float32)
                for q in range(2 * blocks):
                    s, j = divmod(q, blocks)
                    piece = surface[s, g * 8 : (g + 1) * 8, j * LANES : (j + 1) * LANES]
                    found = jnp.where(block == q, take(piece, lanes), found)
                for k in range(LANES // TAIL):
                    move = (LANES - TAIL - k * TAIL) % LANES
                    pieces.append(pltpu.roll(found, move, 1) if move else found)
            tails[g * 8 : (g + 1) * 8] = jnp.swapaxes(jnp.stack(pieces, axis=0), 0, 1)

    def wanted_at(base, t, q):
        row = cell_ref[pl.ds(base, 8), q * LANES : (q + 1) * LANES]
        return spread_row(row[t : t + 1])

    def chosen_from(tile, wanted, start):
        own = tile * 2 * blocks
        block, lanes = wanted >> 7, wanted & (LANES - 1)
        chosen = take(plain[own + start], lanes)
        for b in range(start + 1, 2 * blocks):
            chosen = jnp.where(block == own + b, take(plain[own + b], lanes), chosen)
        return chosen

    def sent(base, group):
        part = pl.ds(base, 8)
        return pltpu.make_async_copy(
            packed.at[part, pl.ds(0, PACKED)], out_ref.at[part, pl.ds(0, PACKED)], sems.at[group]
        )

    def pack(group, _, near):
        base = pl.multiple_of(group * 8, 8)
        for t in range(8):
            tile = base + t
            for q in range(PACKED):
                wanted = wanted_at(base, t, q)
                if near:
                    head = heads[tile, q]
                    b = head >> 7
                    turn = lane_row >= (head & (LANES - 1))
                    low, middle, high = plain[b], plain[b + 1], plain[b + 2]
                    lanes = wanted & (LANES - 1)
                    early = take(jnp.where(turn, low, middle), lanes)
                    late = take(jnp.where(turn, middle, high), lanes)
                    chosen = jnp.where(wanted - head < LANES, early, late)
                else:
                    chosen = chosen_from(tile, wanted, q)
                if field == 0 and q == PACKED - 1:
                    chosen = jnp.where(lane_row >= LANES - TAIL, tails[tile], chosen)
                packed[tile, q] = chosen
        sent(base, group).start()
        return 0

    groups = tiles // 8

    @pl.when(heads[0, PACKED] < 2 * LANES)
    def _():
        lax.fori_loop(0, groups, functools.partial(pack, near=True), 0)

    @pl.when(heads[0, PACKED] >= 2 * LANES)
    def _():
        lax.fori_loop(0, groups, functools.partial(pack, near=False), 0)

    @pl.when(heads[0, PACKED + 1] > 0)
    def _():
        def late_cells(group, _):
            base = pl.multiple_of(group * 8, 8)
            for t in range(8):
                for q in range(PACKED, PACKED + SPILL):
                    packed[base + t, q] = chosen_from(
                        base + t, wanted_at(base, t, q), ROOM // LANES
                    )
            return 0

        lax.fori_loop(0, groups, late_cells, 0)
        copy = pltpu.make_async_copy(
            packed.at[:, pl.ds(PACKED, SPILL)], spill_ref, sems.at[groups]
        )
        copy.start()
        copy.wait()

    for g in range(groups):
        sent(g * 8, g).wait()


def gram_kernel(tile_ref, held_ref, value_ref, error_ref, count_ref, _, out_ref, spread, sem):
    tile = tile_ref[0]
    members = held_ref.shape[0]
    halves = value_ref.shape[2] // LANES
    slot = lax.broadcasted_iota(jnp.int32, (1, LANES), 1)
    total = jnp.zeros((members + 8, members), jnp.float32)
    for h in range(halves):
        seen = jnp.zeros((members, LANES), jnp.float32)
        for k in range(LANES // TAIL):
            piece = held_ref[:, PACKED - 1, h * (LANES // TAIL) + k, :]
            move = (k + 1) * TAIL % LANES
            piece = pltpu.roll(piece, move, 1) if move else piece
            seen = jnp.where((slot >= k * TAIL) & (slot < (k + 1) * TAIL), piece, seen)
        average = jnp.mean(seen, axis=0, keepdims=True)
        anomaly = seen - average
        span = slice(h * LANES, (h + 1) * LANES)
        own = lax.broadcasted_iota(jnp.int32, (value_ref.shape[1], LANES), 0) == tile
        value = jnp.sum(jnp.where(own, value_ref[0, :, span], 0.0), axis=0, keepdims=True)
        error = jnp.sum(jnp.where(own, error_ref[0, :, span], 0.0), axis=0, keepdims=True)
        active = jnp.where(slot + h * LANES < count_ref[0, tile], 1.0, 0.0)
        weight = active / error
        drift = weight * (value - average)
        left = jnp.concatenate([anomaly * weight, jnp.broadcast_to(drift, (8, LANES))], axis=0)
        total = total + lax.dot_general(
            left, anomaly, (((1,), (1,)), ((), ())),
            precision=lax.Precision.HIGHEST, preferred_element_type=jnp.float32,
        )
    packed = jnp.concatenate([total[g * 8 : (g + 1) * 8] for g in range(4)], axis=1)
    pull = jnp.concatenate([total[members : members + 8]] * 4, axis=1)
    row = lax.broadcasted_iota(jnp.int32, packed.shape, 0)
    lane = lax.broadcasted_iota(jnp.int32, packed.shape, 1)
    corner = (lane >= 16) & (lane < 32)
    packed = jnp.where(corner & (row == 0), pltpu.roll(pull, 16, 1), packed)
    packed = jnp.where(corner & (row == 1), pull, packed)
    for m in range(members):
        spread[m, 0] = packed
    copy = pltpu.make_async_copy(spread, out_ref.at[:, pl.ds(PACKED, 1)], sem)
    copy.start()
    copy.wait()


def ensemble_kernel(packed, wide):
    count = 32
    lane = lax.broadcasted_iota(jnp.int32, (count, LANES), 1)
    row = lax.broadcasted_iota(jnp.int32, (count, LANES), 0)
    gram = jnp.concatenate(
        [packed if g == 0 else pltpu.roll(packed, LANES - g * count, 1) for g in range(4)], axis=0
    )
    pull = jnp.where(
        lane[0:1] < 16,
        pltpu.roll(packed[0:8], LANES - 16, 1)[0:1],
        packed[1:2],
    )
    gram = gram + jnp.where(lane == row, count - 1.0, 0.0)
    columns = [jnp.broadcast_to(gram[:, k : k + 1], (count, LANES)) for k in range(count)]
    work = jnp.where(lane == row, 1.0, 0.0)
    for k in range(count):
        base = (k // 8) * 8
        column = columns[k][base:]
        pivot = jnp.broadcast_to(column[k - base : k - base + 1], (8, LANES))
        scale = lax.rsqrt(pivot)
        scale = scale * (1.5 - 0.5 * pivot * scale * scale)
        head = scale[0:1]
        lead = work[k : k + 1] * head
        column = column * head
        below = row[base:] > k
        factor = jnp.where(below, column, 0.0)
        rest = jnp.where(row[base:] == k, lead, work[base:] - factor * lead)
        work = rest if base == 0 else jnp.concatenate([work[:base], rest], axis=0)
        for c in range(k + 1, count):
            cbase = (c // 8) * 8
            ratio = column[c - base : c - base + 1]
            old = columns[c]
            fresh = old[cbase:] - column[cbase - base :] * ratio
            columns[c] = fresh if cbase == 0 else jnp.concatenate([old[:cbase], fresh], axis=0)
    inverse = work
    gained = jnp.sum(inverse * pull, axis=1, keepdims=True)
    mean_weight = jnp.sum(inverse * gained, axis=0, keepdims=True)
    live = lane < count
    weights = jnp.where(live, mean_weight + jnp.sqrt(count - 1.0) * inverse, 0.0)
    centre = jnp.sum(weights, axis=1, keepdims=True) * (1.0 / count)
    return jnp.where(live, weights - centre + 1.0 / count, 0.0)


def mixed(high, low, data):
    major = data.astype(jnp.bfloat16)
    minor = (data - major.astype(jnp.float32)).astype(jnp.bfloat16)
    total = jnp.dot(high[...], major, preferred_element_type=jnp.float32)
    total = total + jnp.dot(high[...], minor, preferred_element_type=jnp.float32)
    return total + jnp.dot(low[...], major, preferred_element_type=jnp.float32)


def mix_strip(high, low, data_ref, at, out_ref, to, blocks):
    members = data_ref.shape[0]
    deep = members * LEVELS
    data = jnp.concatenate(
        [data_ref[:, at + b].reshape(deep, LANES) for b in range(blocks)], axis=1
    )
    result = mixed(high, low, data)
    for b in range(blocks):
        out_ref[:, to + b] = result[:, b * LANES : (b + 1) * LANES].reshape(members, LEVELS, LANES)


def mix_kernel(data0_ref, data1_ref, out_ref, high, low, ready, sems):
    members = data0_ref.shape[0]
    deep = members * LEVELS

    kernel = ensemble_kernel(jnp.sum(data1_ref[:, PACKED], axis=0), LANES)[:, :members]
    major = kernel.astype(jnp.bfloat16)
    minor = (kernel - major.astype(jnp.float32)).astype(jnp.bfloat16)
    spread = (
        lax.broadcasted_iota(jnp.int32, (deep, members), 0) // LEVELS
        == lax.broadcasted_iota(jnp.int32, (deep, members), 1)
    ).astype(jnp.bfloat16)
    same = (
        lax.broadcasted_iota(jnp.int32, (deep, deep), 0) % LEVELS
        == lax.broadcasted_iota(jnp.int32, (deep, deep), 1) % LEVELS
    )
    for part, target in ((major, high), (minor, low)):
        tall = jnp.dot(spread, part, preferred_element_type=jnp.float32).astype(jnp.bfloat16)
        full = lax.dot_general(
            tall, spread, (((1,), (1,)), ((), ())), preferred_element_type=jnp.float32
        )
        target[...] = jnp.where(same, full, 0.0).astype(jnp.bfloat16)

    blocks = 3

    def leaving(to, n):
        part = (slice(None), pl.ds(to, blocks))
        return pltpu.make_async_copy(ready.at[part], out_ref.at[part], sems.at[n])

    for f, data_ref in ((0, data0_ref), (1, data1_ref)):

        def strip(i, _, f=f, data_ref=data_ref):
            at = i * blocks
            to = f * PACKED + at
            mix_strip(high, low, data_ref, at, ready, to, blocks)
            leaving(to, f * (PACKED // blocks) + i).start()
            return 0

        lax.fori_loop(0, PACKED // blocks, strip, 0)
    for n in range(FIELDS * PACKED // blocks):
        leaving(n * blocks, n).wait()


def spill_kernel(data_ref, high, low, out_ref):
    mix_strip(high, low, data_ref, 0, out_ref, 0, data_ref.shape[1])


def settle_rows(spilled, first_ref, back_ref, spill_ref, place_ref, sea_ref, x_ref, out_ref):
    blocks = out_ref.shape[4] // LANES
    start = pl.multiple_of(pl.program_id(0) * 8, 8)
    end = back_ref.shape[0] - 1
    lane_row = lax.broadcasted_iota(jnp.int32, (LEVELS, LANES), 1)

    def take(source, lanes):
        return jnp.take_along_axis(source, lanes, axis=1, mode="promise_in_bounds")

    for j in range(blocks):
        lanes_at = slice(j * LANES, (j + 1) * LANES)
        wanted8 = [
            place_ref[pl.ds(start, 8), b * LANES : (b + 1) * LANES] for b in (j, blocks + j)
        ]
        for half in range(2):
            rows = ([], [])
            for t in range(half * 4, half * 4 + 4):
                for s in range(2):
                    b = s * blocks + j
                    wanted = spread_row(wanted8[s][t : t + 1])
                    block, lanes = wanted >> 7, wanted & (LANES - 1)
                    head = first_ref[start + t, b]
                    at = head >> 7
                    turn = lane_row >= (head & (LANES - 1))
                    for f in range(FIELDS):
                        low = back_ref[at + f * PACKED]
                        high = back_ref[jnp.minimum(at + (f * PACKED + 1), end)]
                        value = take(jnp.where(turn, low, high), lanes)
                        if spilled and (b + 1) * LANES > ROOM:
                            for o in range(SPILL):
                                late = take(spill_ref[start + t, f * SPILL + o], lanes)
                                value = jnp.where(block == PACKED + o, late, value)
                        rows[f].append(value)
            here = pl.ds(pl.multiple_of(2 * start + half * 8, 8), 8)
            there = slice(half * 8, half * 8 + 8)
            ocean = sea_ref[here, lanes_at] > 0.0
            for f in range(FIELDS):
                turned = jnp.swapaxes(jnp.stack(rows[f], axis=0), 0, 1)
                for l in range(LEVELS):
                    out_ref[0, f, l, there, lanes_at] = jnp.where(
                        ocean, turned[l], x_ref[0, f, l, here, lanes_at]
                    )


def settle_kernel(first_ref, *refs):
    late = first_ref[0, LANES - 1] > 0

    @pl.when(late)
    def _():
        settle_rows(True, first_ref, *refs)

    @pl.when(jnp.logical_not(late))
    def _():
        settle_rows(False, first_ref, *refs)


def shards(
    starting_tracer_fields,
    surface_exchange_inputs,
    diffusivity,
    mixing,
    land_mask,
    obs_index,
    obs_count,
    obs_value,
    obs_error,
):
    _, fields, levels, rows, width = starting_tracer_fields.shape
    members = lax.axis_size("member")
    domains = lax.axis_size("domain")
    blocks = width // LANES
    tiles = members
    per_field = 2 * blocks
    tile = lax.axis_index("member")
    domain = lax.axis_index("domain")
    state, flux = starting_tracer_fields[0], surface_exchange_inputs[0]

    def edge(first, flux_row):
        lines = jnp.swapaxes(state[:, :, first : first + HALO], 1, 2)
        lines = lines.reshape(fields, HALO * levels, width)
        return jnp.concatenate([lines, flux[:, flux_row : flux_row + 1]], axis=1)

    up = [(i, i + 1) for i in range(domains - 1)]
    down = [(i + 1, i) for i in range(domains - 1)]
    before = lax.ppermute(edge(rows - HALO, rows - 1), "domain", up)
    after = lax.ppermute(edge(0, 0), "domain", down)

    padded = jnp.pad(land_mask, ((HALO, HALO), (0, 0)))
    mask = lax.dynamic_slice_in_dim(padded, domain * rows, rows + 2 * HALO, 0).astype(jnp.float32)

    f32 = jnp.float32
    tall = rows + 2 * HALO
    vmem = pl.BlockSpec(memory_space=pltpu.VMEM)
    smem = pl.BlockSpec(memory_space=pltpu.SMEM)
    anywhere = pl.BlockSpec(memory_space=pl.ANY)
    hbm = pl.BlockSpec(memory_space=pltpu.HBM)

    def params(mib):
        return pltpu.CompilerParams(vmem_limit_bytes=mib << 20)

    band = jax.ShapeDtypeStruct((rows, levels, width), f32)
    shell = jax.ShapeDtypeStruct((tall, levels, width), f32)
    i32 = jnp.int32
    bulks = [pltpu.HBM((tiles, PACKED + f, levels, LANES), f32) for f in range(2)]
    extra = pltpu.HBM((tiles, SPILL, levels, LANES), f32)
    mark = jax.ShapeDtypeStruct((levels, LANES), f32)

    cell, place, first, heads, sea = pl.pallas_call(
        survey_kernel,
        out_shape=[
            jax.ShapeDtypeStruct((tiles, (PACKED + SPILL) * LANES), i32),
            pltpu.HBM((tiles, 2 * width), i32),
            pltpu.HBM((tiles, LANES), i32),
            jax.ShapeDtypeStruct((tiles, LANES), i32),
            pltpu.HBM((rows, width), f32),
        ],
        in_specs=[vmem],
        out_specs=[vmem] * 5,
        compiler_params=params(8),
        cost_estimate=pl.CostEstimate(
            flops=20_000_000, bytes_accessed=500_000, transcendentals=0
        ),
        name="survey",
    )(mask)

    def prepare(field, *after_this):
        return pl.pallas_call(
            functools.partial(prepare_kernel, field),
            out_shape=[band, band, band, shell, shell],
            in_specs=[hbm, vmem, vmem] + [anywhere] * len(after_this),
            out_specs=[vmem] * 5,
            scratch_shapes=[
                pltpu.VMEM((levels, rows, width), f32),
                pltpu.SemaphoreType.DMA((rows // 8,)),
            ],
            compiler_params=params(8),
            cost_estimate=pl.CostEstimate(
                flops=20_000_000, bytes_accessed=3_000_000, transcendentals=0
            ),
            name=f"prepare_{field}",
        )(
            pltpu.with_memory_space_constraint(starting_tracer_fields, pltpu.HBM),
            surface_exchange_inputs, mask, *after_this,
        )

    def forecast(field, prepared, *inputs):
        scratch = [
            pltpu.VMEM((tall, levels, width), f32),
            pltpu.VMEM((tall, levels, width), f32),
            pltpu.VMEM((tiles * per_field + 2, levels, LANES), f32),
            pltpu.VMEM((tiles, PACKED + SPILL, levels, LANES), f32),
            pltpu.SMEM((tiles, LANES), i32),
            pltpu.SemaphoreType.DMA((tiles // 8 + 1,)),
        ]
        out_shape = [bulks[field], extra]
        out_specs = [hbm] * 2
        if field == 0:
            scratch.append(pltpu.VMEM((2, tiles, width), f32))
            scratch.append(pltpu.VMEM((tiles, levels, LANES), f32))
            out_shape.append(mark)
            out_specs.append(vmem)
        return pl.pallas_call(
            functools.partial(forecast_kernel, field),
            out_shape=out_shape,
            in_specs=[vmem] * (11 + len(inputs)),
            out_specs=out_specs,
            scratch_shapes=scratch,
            compiler_params=params(10),
            cost_estimate=pl.CostEstimate(
                flops=40_000_000, bytes_accessed=3_000_000, transcendentals=0
            ),
            name=f"forecast_{field}",
        )(*prepared, before, after, diffusivity, mixing, cell, heads, *inputs)

    def exchanged(array):
        return lax.all_to_all(array, "member", split_axis=0, concat_axis=0, tiled=True)

    sent0, spill0, done0 = forecast(0, prepare(0), obs_index)
    held0 = exchanged(sent0)
    sent1, spill1 = forecast(1, prepare(1, done0))
    sent1 = pl.pallas_call(
        gram_kernel,
        out_shape=bulks[1],
        in_specs=[smem, vmem, vmem, vmem, smem, hbm],
        out_specs=hbm,
        scratch_shapes=[
            pltpu.VMEM((tiles, 1, levels, LANES), f32),
            pltpu.SemaphoreType.DMA,
        ],
        input_output_aliases={5: 0},
        compiler_params=params(4),
        name="gram",
    )(tile.reshape(1).astype(jnp.int32), held0, obs_value, obs_error, obs_count, sent1)
    held1 = exchanged(sent1)

    deep = members * levels
    half = jax.ShapeDtypeStruct((deep, deep), jnp.bfloat16)
    updated, high, low = pl.pallas_call(
        mix_kernel,
        out_shape=[
            pltpu.HBM((members, fields * PACKED, levels, LANES), f32), half, half
        ],
        in_specs=[vmem, vmem],
        out_specs=[hbm, vmem, vmem],
        scratch_shapes=[
            pltpu.VMEM((members, fields * PACKED, levels, LANES), f32),
            pltpu.SemaphoreType.DMA((fields * PACKED // 3,)),
        ],
        compiler_params=params(16),
        name="mix",
    )(held0, held1)
    back = exchanged(updated)

    def late(spill, high, low):
        there = exchanged(spill)
        there = pl.pallas_call(
            spill_kernel,
            out_shape=jax.ShapeDtypeStruct(there.shape, f32),
            in_specs=[vmem] * 3,
            out_specs=vmem,
            compiler_params=params(16),
            name="mix_spill",
        )(there, high, low)
        return exchanged(there)

    def none(spill, high, low):
        return spill

    ocean = jnp.sum(land_mask, axis=1).reshape(-1, 2).sum(axis=1)
    spill = jnp.concatenate([spill0, spill1], axis=1)
    spill = lax.cond(jnp.max(ocean) > ROOM, late, none, spill, high, low)

    bands = pl.BlockSpec((1, fields, levels, 16, width), lambda i: (0, 0, 0, i, 0))
    return pl.pallas_call(
        settle_kernel,
        grid=(rows // 16,),
        out_shape=jax.ShapeDtypeStruct(starting_tracer_fields.shape, f32),
        in_specs=[smem] + [vmem] * 5,
        out_specs=bands,
        compiler_params=params(12),
        name="settle",
    )(
        first, back.reshape(-1, levels, LANES), spill, place, sea, starting_tracer_fields,
    )


def solution(mesh):
    placed = (
        P("member", None, None, "domain", None),
        P("member", None, "domain", None),
        P(),
        P(),
        P(),
        P("domain", None, None),
        P("domain", None),
        P("domain", None, None),
        P("domain", None, None),
    )
    return jax.shard_map(
        shards,
        mesh=mesh,
        in_specs=placed,
        out_specs=P("member", None, None, "domain", None),
        check_vma=False,
    )
```

```python
import functools

import jax
import jax.numpy as jnp
from jax import lax
from jax.experimental import pallas as pl
from jax.experimental.pallas import tpu as pltpu
from jax.sharding import PartitionSpec as P

FIELDS = 2
LEVELS = 8
LANES = 128
HALO = 2
UNROLL = 10
PACKED = 9
TAIL = 32
ROOM = PACKED * LANES - TAIL
SPILL = 2


def spread_row(row):
    return jnp.broadcast_to(row, (LEVELS, row.shape[1]))


def ranked(mask_ref, tiles, cells):
    rows = 2 * tiles
    blocks = cells // LANES
    sea = mask_ref[HALO : HALO + rows, :].astype(jnp.bfloat16)
    pick = lax.broadcasted_iota(jnp.int32, (tiles, rows), 1) - 2 * lax.broadcasted_iota(
        jnp.int32, (tiles, rows), 0
    )
    sides = [
        jnp.dot((pick == s).astype(jnp.bfloat16), sea, preferred_element_type=jnp.float32)
        for s in range(2)
    ]
    sea = jnp.concatenate(sides, axis=1)
    land = (1.0 - sea).astype(jnp.bfloat16)
    stacked = jnp.concatenate([land[:, b * LANES : (b + 1) * LANES] for b in range(blocks)], axis=0)
    before = (
        lax.broadcasted_iota(jnp.int32, (LANES, LANES), 0)
        < lax.broadcasted_iota(jnp.int32, (LANES, LANES), 1)
    ).astype(jnp.bfloat16)
    within = jnp.dot(stacked, before, preferred_element_type=jnp.float32)
    totals = jnp.dot(
        stacked, jnp.ones((LANES, LANES), jnp.bfloat16), preferred_element_type=jnp.float32
    )
    offset = jnp.zeros((tiles, LANES), jnp.float32)
    shifts = []
    for b in range(blocks):
        part = slice(b * tiles, (b + 1) * tiles)
        shifts.append(within[part] + offset)
        offset = offset + totals[part]
    return sea, jnp.concatenate(shifts, axis=1).astype(jnp.int32)


def placed_cells(sea, shift):
    rank = lax.broadcasted_iota(jnp.int32, shift.shape, 1) - shift
    place = jnp.where(rank < ROOM, rank, rank + TAIL)
    return place, jnp.where(sea > 0.0, place, -1)


def spilling(marked, shape):
    last = jnp.max(jnp.max(marked, axis=1, keepdims=True), axis=0, keepdims=True)
    return (jnp.broadcast_to(last, shape) >= PACKED * LANES).astype(jnp.int32)


def locate_kernel(mask_ref, _, place_ref, first_ref, sea_ref):
    tiles, cells = place_ref.shape
    sea_ref[...] = mask_ref[HALO : HALO + 2 * tiles, :]
    place, marked = placed_cells(*ranked(mask_ref, tiles, cells))
    place_ref[...] = marked
    lane = lax.broadcasted_iota(jnp.int32, first_ref.shape, 1)
    first = jnp.zeros(first_ref.shape, jnp.int32)
    for b in range(cells // LANES):
        head = place[:, b * LANES : b * LANES + 1]
        head = (jnp.minimum(head >> 7, PACKED - 1) << 7) + (head & (LANES - 1))
        first = jnp.where(lane == b, jnp.broadcast_to(head, first.shape), first)
    number = lax.broadcasted_iota(jnp.int32, first.shape, 0)
    first = first + number * (FIELDS * PACKED * LANES)
    first_ref[...] = jnp.where(lane == LANES - 1, spilling(marked, first.shape), first)


def survey_kernel(mask_ref, cell_ref, head_ref):
    tiles, cells = cell_ref.shape[0], 2 * mask_ref.shape[1]
    sea, shift = ranked(mask_ref, tiles, cells)
    cell = lax.broadcasted_iota(jnp.int32, shift.shape, 1)
    state = jnp.where(sea > 0.0, shift * 2048 + cell, 0)
    for bit in range(11):
        other = pltpu.roll(state, cells - (1 << bit), 1)
        comes = (other & (2048 << bit)) != 0
        goes = (state & (2048 << bit)) != 0
        state = jnp.where(comes, other, jnp.where(goes, 0, state))
    state = state & 2047
    heads = jnp.zeros(head_ref.shape, jnp.int32)
    lane = lax.broadcasted_iota(jnp.int32, heads.shape, 1)
    number = lax.broadcasted_iota(jnp.int32, heads.shape, 0)
    reach = jnp.zeros((tiles, 1), jnp.int32)
    for q in range(PACKED):
        part = state[:, q * LANES : (q + 1) * LANES]
        heads = jnp.where(lane == q, jnp.broadcast_to(part[:, 0:1], heads.shape), heads)
        reach = jnp.maximum(reach, jnp.max(part, axis=1, keepdims=True) - part[:, 0:1])
    wide = jnp.max(reach, axis=0, keepdims=True)
    heads = heads + number * cells
    heads = jnp.where(lane == PACKED, jnp.broadcast_to(wide, heads.shape), heads)
    _, marked = placed_cells(sea, shift)
    head_ref[...] = jnp.where(lane == PACKED + 1, spilling(marked, heads.shape), heads)
    state = state + lax.broadcasted_iota(jnp.int32, state.shape, 0) * cells
    cell_ref[:, : PACKED * LANES] = state[:, : PACKED * LANES]
    cell_ref[:, PACKED * LANES :] = pltpu.roll(state, cells - ROOM, 1)[:, : SPILL * LANES]


def prepare_kernel(field, x_ref, flux_ref, mask_ref, *rest):
    turned, wet, source, sea8, crowd8, held, sems = rest[-7:]
    rows, width = turned.shape[0], turned.shape[2]
    tall = rows + 2 * HALO
    parts = rows // 8
    copies = []
    for p in range(parts):
        span = pl.ds(p * 8, 8)
        copy = pltpu.make_async_copy(
            x_ref.at[0, field, :, span, :], held.at[:, span, :], sems.at[p]
        )
        copy.start()
        copies.append(copy)
    sea = mask_ref[1 : tall - 1, :]
    crowd = (
        mask_ref[0 : tall - 2, :] + mask_ref[2:tall, :]
        + pltpu.roll(sea, 1, 1) + pltpu.roll(sea, width - 1, 1)
    )
    for r in range(tall):
        sea8[r] = spread_row(mask_ref[r : r + 1, :])
    for r in range(1, tall - 1):
        crowd8[r] = spread_row(crowd[r - 1 : r, :])
    top = lax.broadcasted_iota(jnp.int32, (LEVELS, width), 0) == 0
    for p in range(parts):
        copies[p].wait()
        start = p * 8
        flipped = jnp.swapaxes(held[:, start : start + 8, :], 0, 1)
        for k in range(8):
            r = start + k
            turned[r] = flipped[k]
            wet[r] = flipped[k] * sea8[r + HALO]
            source[r] = jnp.where(top, spread_row(flux_ref[0, field, r : r + 1, :]), 0.0)


def forecast_kernel(field, turned, wet, source, sea8, crowd8, before_ref, after_ref,
                    diff_ref, mix_ref, *rest):
    cell_ref, head_ref, rest = rest[0], rest[1], rest[2:]
    if field == 0:
        index_ref, out_ref, spill_ref, done_ref, first, moist, plain, packed, heads, sems, surface, tails = rest
        done_ref[...] = jnp.zeros_like(done_ref)
    else:
        out_ref, spill_ref, first, moist, plain, packed, heads, sems = rest
    table = pltpu.make_async_copy(head_ref, heads, sems.at[0])
    table.start()
    rows, width = turned.shape[0], turned.shape[2]
    tall = rows + 2 * HALO
    blocks = width // LANES

    level = lax.broadcasted_iota(jnp.int32, (LEVELS, LEVELS), 0)
    lane = lax.broadcasted_iota(jnp.int32, (LEVELS, LEVELS), 1)
    diff = diff_ref[field : field + 1, :]
    mix = jnp.concatenate([mix_ref[field : field + 1, :], jnp.zeros((1, 1), jnp.float32)], axis=1)

    def along(table, shift):
        column = jnp.sum(jnp.where(lane + shift == level, table, 0.0), axis=1, keepdims=True)
        return jnp.concatenate([jnp.broadcast_to(column, (LEVELS, LANES))] * blocks, axis=1)

    lateral, above, below = along(diff, 0), along(mix, 0), along(mix, 1)
    vertical = above + below

    def stepped(r, x, y, north, south, gain):
        sea = sea8[r]
        around = north + south + pltpu.roll(y, 1, 1) + pltpu.roll(y, width - 1, 1)
        change = lateral * (around - crowd8[r] * x) - vertical * x + gain
        change = change + above * pltpu.roll(x, LEVELS - 1, 0)
        change = change + below * pltpu.roll(x, 1, 0)
        return x + sea * change

    def near(r):
        if r < HALO:
            x = before_ref[field, r * LEVELS : (r + 1) * LEVELS, :]
        elif r >= HALO + rows:
            h = r - HALO - rows
            x = after_ref[field, h * LEVELS : (h + 1) * LEVELS, :]
        else:
            return turned[r - HALO], wet[r - HALO]
        return x, x * sea8[r]

    top = lax.broadcasted_iota(jnp.int32, (LEVELS, width), 0) == 0

    def gain_at(r):
        if HALO <= r < HALO + rows:
            return source[r - HALO]
        ref = before_ref if r < HALO else after_ref
        line = ref[field, HALO * LEVELS : HALO * LEVELS + 1, :]
        return jnp.where(top, spread_row(line), 0.0)

    def keep(r, value):
        first[r] = value
        moist[r] = value * sea8[r]

    def inner(r, _):
        i = r - HALO
        keep(r, stepped(r, turned[i], wet[i], wet[i - 1], wet[i + 1], source[i]))
        return 0

    body = (tall - 6) // UNROLL * UNROLL
    for r in (1, 2, *range(3 + body, tall - 1)):
        x, y = near(r)
        keep(r, stepped(r, x, y, near(r - 1)[1], near(r + 1)[1], gain_at(r)))
    lax.fori_loop(3, 3 + body, inner, 0, unroll=UNROLL)

    def outer(tile, _):
        for side in range(2):
            r = HALO + 2 * tile + side
            value = stepped(r, first[r], moist[r], moist[r - 1], moist[r + 1], source[r - HALO])
            for j in range(blocks):
                plain[tile * 2 * blocks + side * blocks + j] = value[:, j * LANES : (j + 1) * LANES]
            if field == 0:
                surface[side, pl.ds(tile, 1), :] = value[0:1, :]
        return 0

    tiles = rows // 2
    lax.fori_loop(0, tiles, outer, 0, unroll=4)
    table.wait()
    lane_row = lax.broadcasted_iota(jnp.int32, (LEVELS, LANES), 1)

    def take(piece, lanes):
        return jnp.take_along_axis(piece, lanes, axis=1, mode="promise_in_bounds")

    if field == 0:
        slots = index_ref.shape[2]
        for g in range(tiles // 8):
            pieces = []
            for h in range(slots // LANES):
                where = index_ref[0, g * 8 : (g + 1) * 8, h * LANES : (h + 1) * LANES]
                block, lanes = where >> 7, where & (LANES - 1)
                found = jnp.zeros((8, LANES), jnp.float32)
                for q in range(2 * blocks):
                    s, j = divmod(q, blocks)
                    piece = surface[s, g * 8 : (g + 1) * 8, j * LANES : (j + 1) * LANES]
                    found = jnp.where(block == q, take(piece, lanes), found)
                for k in range(LANES // TAIL):
                    move = (LANES - TAIL - k * TAIL) % LANES
                    pieces.append(pltpu.roll(found, move, 1) if move else found)
            tails[g * 8 : (g + 1) * 8] = jnp.swapaxes(jnp.stack(pieces, axis=0), 0, 1)

    def wanted_at(base, t, q):
        row = cell_ref[pl.ds(base, 8), q * LANES : (q + 1) * LANES]
        return spread_row(row[t : t + 1])

    def chosen_from(tile, wanted, start):
        own = tile * 2 * blocks
        block, lanes = wanted >> 7, wanted & (LANES - 1)
        chosen = take(plain[own + start], lanes)
        for b in range(start + 1, 2 * blocks):
            chosen = jnp.where(block == own + b, take(plain[own + b], lanes), chosen)
        return chosen

    def sent(base, group):
        part = pl.ds(base, 8)
        return pltpu.make_async_copy(
            packed.at[part, pl.ds(0, PACKED)], out_ref.at[part, pl.ds(0, PACKED)], sems.at[group]
        )

    def pack(group, _, near):
        base = pl.multiple_of(group * 8, 8)
        for t in range(8):
            tile = base + t
            for q in range(PACKED):
                wanted = wanted_at(base, t, q)
                if near:
                    head = heads[tile, q]
                    b = head >> 7
                    turn = lane_row >= (head & (LANES - 1))
                    low, middle, high = plain[b], plain[b + 1], plain[b + 2]
                    lanes = wanted & (LANES - 1)
                    early = take(jnp.where(turn, low, middle), lanes)
                    late = take(jnp.where(turn, middle, high), lanes)
                    chosen = jnp.where(wanted - head < LANES, early, late)
                else:
                    chosen = chosen_from(tile, wanted, q)
                if field == 0 and q == PACKED - 1:
                    chosen = jnp.where(lane_row >= LANES - TAIL, tails[tile], chosen)
                packed[tile, q] = chosen
        sent(base, group).start()
        return 0

    groups = tiles // 8

    @pl.when(heads[0, PACKED] < 2 * LANES)
    def _():
        lax.fori_loop(0, groups, functools.partial(pack, near=True), 0)

    @pl.when(heads[0, PACKED] >= 2 * LANES)
    def _():
        lax.fori_loop(0, groups, functools.partial(pack, near=False), 0)

    @pl.when(heads[0, PACKED + 1] > 0)
    def _():
        def late_cells(group, _):
            base = pl.multiple_of(group * 8, 8)
            for t in range(8):
                for q in range(PACKED, PACKED + SPILL):
                    packed[base + t, q] = chosen_from(
                        base + t, wanted_at(base, t, q), ROOM // LANES
                    )
            return 0

        lax.fori_loop(0, groups, late_cells, 0)
        copy = pltpu.make_async_copy(
            packed.at[:, pl.ds(PACKED, SPILL)], spill_ref, sems.at[groups]
        )
        copy.start()
        copy.wait()

    for g in range(groups):
        sent(g * 8, g).wait()


def gram_kernel(
    tile_ref, held_ref, value_ref, error_ref, count_ref, _, out_ref, sums_ref, spread, sem
):
    tile = tile_ref[0]
    members = held_ref.shape[0]
    halves = value_ref.shape[2] // LANES
    slot = lax.broadcasted_iota(jnp.int32, (1, LANES), 1)
    total = jnp.zeros((members + 8, members), jnp.float32)
    for h in range(halves):
        seen = jnp.zeros((members, LANES), jnp.float32)
        for k in range(LANES // TAIL):
            piece = held_ref[:, PACKED - 1, h * (LANES // TAIL) + k, :]
            move = (k + 1) * TAIL % LANES
            piece = pltpu.roll(piece, move, 1) if move else piece
            seen = jnp.where((slot >= k * TAIL) & (slot < (k + 1) * TAIL), piece, seen)
        average = jnp.mean(seen, axis=0, keepdims=True)
        anomaly = seen - average
        span = slice(h * LANES, (h + 1) * LANES)
        own = lax.broadcasted_iota(jnp.int32, (value_ref.shape[1], LANES), 0) == tile
        value = jnp.sum(jnp.where(own, value_ref[0, :, span], 0.0), axis=0, keepdims=True)
        error = jnp.sum(jnp.where(own, error_ref[0, :, span], 0.0), axis=0, keepdims=True)
        active = jnp.where(slot + h * LANES < count_ref[0, tile], 1.0, 0.0)
        weight = active / error
        drift = weight * (value - average)
        left = jnp.concatenate([anomaly * weight, jnp.broadcast_to(drift, (8, LANES))], axis=0)
        total = total + lax.dot_general(
            left, anomaly, (((1,), (1,)), ((), ())),
            precision=lax.Precision.HIGHEST, preferred_element_type=jnp.float32,
        )
    packed = jnp.concatenate([total[g * 8 : (g + 1) * 8] for g in range(4)], axis=1)
    pull = jnp.concatenate([total[members : members + 8]] * 4, axis=1)
    row = lax.broadcasted_iota(jnp.int32, packed.shape, 0)
    lane = lax.broadcasted_iota(jnp.int32, packed.shape, 1)
    corner = (lane >= 16) & (lane < 32)
    packed = jnp.where(corner & (row == 0), pltpu.roll(pull, 16, 1), packed)
    packed = jnp.where(corner & (row == 1), pull, packed)
    sums_ref[...] = packed
    for m in range(members):
        spread[m, 0] = packed
    copy = pltpu.make_async_copy(spread, out_ref.at[:, pl.ds(PACKED, 1)], sem)
    copy.start()
    copy.wait()


def ensemble_kernel(packed, wide):
    count = 32
    lane = lax.broadcasted_iota(jnp.int32, (count, LANES), 1)
    row = lax.broadcasted_iota(jnp.int32, (count, LANES), 0)
    gram = jnp.concatenate(
        [packed if g == 0 else pltpu.roll(packed, LANES - g * count, 1) for g in range(4)], axis=0
    )
    pull = jnp.where(
        lane[0:1] < 16,
        pltpu.roll(packed[0:8], LANES - 16, 1)[0:1],
        packed[1:2],
    )
    gram = gram + jnp.where(lane == row, count - 1.0, 0.0)
    columns = [jnp.broadcast_to(gram[:, k : k + 1], (count, LANES)) for k in range(count)]
    work = jnp.where(lane == row, 1.0, 0.0)
    for k in range(count):
        base = (k // 8) * 8
        column = columns[k][base:]
        pivot = jnp.broadcast_to(column[k - base : k - base + 1], (8, LANES))
        scale = lax.rsqrt(pivot)
        scale = scale * (1.5 - 0.5 * pivot * scale * scale)
        head = scale[0:1]
        lead = work[k : k + 1] * head
        column = column * head
        below = row[base:] > k
        factor = jnp.where(below, column, 0.0)
        rest = jnp.where(row[base:] == k, lead, work[base:] - factor * lead)
        work = rest if base == 0 else jnp.concatenate([work[:base], rest], axis=0)
        for c in range(k + 1, count):
            cbase = (c // 8) * 8
            ratio = column[c - base : c - base + 1]
            old = columns[c]
            fresh = old[cbase:] - column[cbase - base :] * ratio
            columns[c] = fresh if cbase == 0 else jnp.concatenate([old[:cbase], fresh], axis=0)
    inverse = work
    gained = jnp.sum(inverse * pull, axis=1, keepdims=True)
    mean_weight = jnp.sum(inverse * gained, axis=0, keepdims=True)
    live = lane < count
    weights = jnp.where(live, mean_weight + jnp.sqrt(count - 1.0) * inverse, 0.0)
    centre = jnp.sum(weights, axis=1, keepdims=True) * (1.0 / count)
    return jnp.where(live, weights - centre + 1.0 / count, 0.0)


def mixed(high, low, data):
    major = data.astype(jnp.bfloat16)
    minor = (data - major.astype(jnp.float32)).astype(jnp.bfloat16)
    total = jnp.dot(high[...], major, preferred_element_type=jnp.float32)
    total = total + jnp.dot(high[...], minor, preferred_element_type=jnp.float32)
    return total + jnp.dot(low[...], major, preferred_element_type=jnp.float32)


def mix_strip(high, low, data_ref, at, out_ref, to, blocks):
    members = data_ref.shape[0]
    deep = members * LEVELS
    data = jnp.concatenate(
        [data_ref[:, at + b].reshape(deep, LANES) for b in range(blocks)], axis=1
    )
    result = mixed(high, low, data)
    for b in range(blocks):
        out_ref[:, to + b] = result[:, b * LANES : (b + 1) * LANES].reshape(members, LEVELS, LANES)


def widen(total, high, low):
    members = total.shape[1] // 4
    deep = members * LEVELS
    kernel = ensemble_kernel(total, LANES)[:, :members]
    major = kernel.astype(jnp.bfloat16)
    minor = (kernel - major.astype(jnp.float32)).astype(jnp.bfloat16)
    spread = (
        lax.broadcasted_iota(jnp.int32, (deep, members), 0) // LEVELS
        == lax.broadcasted_iota(jnp.int32, (deep, members), 1)
    ).astype(jnp.bfloat16)
    same = (
        lax.broadcasted_iota(jnp.int32, (deep, deep), 0) % LEVELS
        == lax.broadcasted_iota(jnp.int32, (deep, deep), 1) % LEVELS
    )
    for part, target in ((major, high), (minor, low)):
        tall = jnp.dot(spread, part, preferred_element_type=jnp.float32).astype(jnp.bfloat16)
        full = lax.dot_general(
            tall, spread, (((1,), (1,)), ((), ())), preferred_element_type=jnp.float32
        )
        target[...] = jnp.where(same, full, 0.0).astype(jnp.bfloat16)


def mix_kernel(data0_ref, data1_ref, out_ref, high, low):
    widen(jnp.sum(data1_ref[:, PACKED], axis=0), high, low)
    blocks = 3
    for f, data_ref in ((0, data0_ref), (1, data1_ref)):

        def strip(i, _, f=f, data_ref=data_ref):
            at = i * blocks
            mix_strip(high, low, data_ref, at, out_ref, f * PACKED + at, blocks)
            return 0

        lax.fori_loop(0, PACKED // blocks, strip, 0)


def spill_kernel(sums_ref, data_ref, out_ref, high, low):
    widen(jnp.sum(sums_ref[:, 0], axis=0), high, low)
    mix_strip(high, low, data_ref, 0, out_ref, 0, data_ref.shape[1])


def census_kernel(mask_ref, _, most_ref):
    rows = jnp.sum(mask_ref[...].astype(jnp.float32), axis=1, keepdims=True)
    rows = jnp.broadcast_to(rows, (rows.shape[0], LANES))
    pairs = rows + pltpu.roll(rows, rows.shape[0] - 1, 0)
    even = lax.broadcasted_iota(jnp.int32, pairs.shape, 0) % 2 == 0
    most = jnp.max(jnp.where(even, pairs, 0.0), axis=0, keepdims=True)
    most_ref[...] = jnp.broadcast_to(most, most_ref.shape)


def settle_rows(
    spilled, first_ref, back_ref, spill0_ref, spill1_ref, place_ref, sea_ref, x_ref, out_ref
):
    blocks = out_ref.shape[4] // LANES
    start = pl.multiple_of(pl.program_id(0) * 8, 8)
    end = back_ref.shape[0] - 1
    lane_row = lax.broadcasted_iota(jnp.int32, (LEVELS, LANES), 1)

    def take(source, lanes):
        return jnp.take_along_axis(source, lanes, axis=1, mode="promise_in_bounds")

    for j in range(blocks):
        lanes_at = slice(j * LANES, (j + 1) * LANES)
        wanted8 = [
            place_ref[pl.ds(start, 8), b * LANES : (b + 1) * LANES] for b in (j, blocks + j)
        ]
        for half in range(2):
            rows = ([], [])
            for t in range(half * 4, half * 4 + 4):
                for s in range(2):
                    b = s * blocks + j
                    wanted = spread_row(wanted8[s][t : t + 1])
                    block, lanes = wanted >> 7, wanted & (LANES - 1)
                    head = first_ref[start + t, b]
                    at = head >> 7
                    turn = lane_row >= (head & (LANES - 1))
                    for f in range(FIELDS):
                        low = back_ref[at + f * PACKED]
                        high = back_ref[jnp.minimum(at + (f * PACKED + 1), end)]
                        value = take(jnp.where(turn, low, high), lanes)
                        if spilled and (b + 1) * LANES > ROOM:
                            for o in range(SPILL):
                                late = take((spill0_ref, spill1_ref)[f][start + t, o], lanes)
                                value = jnp.where(block == PACKED + o, late, value)
                        rows[f].append(value)
            here = pl.ds(pl.multiple_of(2 * start + half * 8, 8), 8)
            there = slice(half * 8, half * 8 + 8)
            ocean = sea_ref[here, lanes_at] > 0.0
            for f in range(FIELDS):
                turned = jnp.swapaxes(jnp.stack(rows[f], axis=0), 0, 1)
                for l in range(LEVELS):
                    out_ref[0, f, l, there, lanes_at] = jnp.where(
                        ocean, turned[l], x_ref[0, f, l, here, lanes_at]
                    )


def settle_kernel(first_ref, *refs):
    late = first_ref[0, LANES - 1] > 0

    @pl.when(late)
    def _():
        settle_rows(True, first_ref, *refs)

    @pl.when(jnp.logical_not(late))
    def _():
        settle_rows(False, first_ref, *refs)


def shards(
    starting_tracer_fields,
    surface_exchange_inputs,
    diffusivity,
    mixing,
    land_mask,
    obs_index,
    obs_count,
    obs_value,
    obs_error,
):
    _, fields, levels, rows, width = starting_tracer_fields.shape
    members = lax.axis_size("member")
    domains = lax.axis_size("domain")
    blocks = width // LANES
    tiles = members
    per_field = 2 * blocks
    tile = lax.axis_index("member")
    domain = lax.axis_index("domain")
    state, flux = starting_tracer_fields[0], surface_exchange_inputs[0]

    def edge(first, flux_row):
        lines = jnp.swapaxes(state[:, :, first : first + HALO], 1, 2)
        lines = lines.reshape(fields, HALO * levels, width)
        return jnp.concatenate([lines, flux[:, flux_row : flux_row + 1]], axis=1)

    up = [(i, i + 1) for i in range(domains - 1)]
    down = [(i + 1, i) for i in range(domains - 1)]
    before = lax.ppermute(edge(rows - HALO, rows - 1), "domain", up)
    after = lax.ppermute(edge(0, 0), "domain", down)

    padded = jnp.pad(land_mask, ((HALO, HALO), (0, 0)))
    mask = lax.dynamic_slice_in_dim(padded, domain * rows, rows + 2 * HALO, 0).astype(jnp.float32)

    f32 = jnp.float32
    tall = rows + 2 * HALO
    vmem = pl.BlockSpec(memory_space=pltpu.VMEM)
    smem = pl.BlockSpec(memory_space=pltpu.SMEM)
    anywhere = pl.BlockSpec(memory_space=pl.ANY)
    hbm = pl.BlockSpec(memory_space=pltpu.HBM)

    def params(mib):
        return pltpu.CompilerParams(vmem_limit_bytes=mib << 20)

    band = jax.ShapeDtypeStruct((rows, levels, width), f32)
    shell = jax.ShapeDtypeStruct((tall, levels, width), f32)
    i32 = jnp.int32
    bulks = [
        pltpu.HBM((tiles, PACKED, levels, LANES), f32),
        jax.ShapeDtypeStruct((tiles, PACKED + 1, levels, LANES), f32),
    ]
    extra = pltpu.HBM((tiles, SPILL, levels, LANES), f32)
    mark = jax.ShapeDtypeStruct((levels, LANES), f32)

    cell, heads = pl.pallas_call(
        survey_kernel,
        out_shape=[
            jax.ShapeDtypeStruct((tiles, (PACKED + SPILL) * LANES), i32),
            jax.ShapeDtypeStruct((tiles, LANES), i32),
        ],
        in_specs=[vmem],
        out_specs=[vmem] * 2,
        compiler_params=params(8),
        cost_estimate=pl.CostEstimate(
            flops=20_000_000, bytes_accessed=500_000, transcendentals=0
        ),
        name="survey",
    )(mask)

    def prepare(field, *after_this):
        return pl.pallas_call(
            functools.partial(prepare_kernel, field),
            out_shape=[band, band, band, shell, shell],
            in_specs=[hbm, vmem, vmem] + [anywhere] * len(after_this),
            out_specs=[vmem] * 5,
            scratch_shapes=[
                pltpu.VMEM((levels, rows, width), f32),
                pltpu.SemaphoreType.DMA((rows // 8,)),
            ],
            compiler_params=params(8),
            cost_estimate=pl.CostEstimate(
                flops=20_000_000, bytes_accessed=3_000_000, transcendentals=0
            ),
            name=f"prepare_{field}",
        )(
            pltpu.with_memory_space_constraint(starting_tracer_fields, pltpu.HBM),
            surface_exchange_inputs, mask, *after_this,
        )

    def forecast(field, prepared, *inputs):
        scratch = [
            pltpu.VMEM((tall, levels, width), f32),
            pltpu.VMEM((tall, levels, width), f32),
            pltpu.VMEM((tiles * per_field + 2, levels, LANES), f32),
            pltpu.VMEM((tiles, PACKED + SPILL, levels, LANES), f32),
            pltpu.SMEM((tiles, LANES), i32),
            pltpu.SemaphoreType.DMA((tiles // 8 + 1,)),
        ]
        out_shape = [bulks[field], extra]
        out_specs = [hbm if field == 0 else anywhere, hbm]
        if field == 0:
            scratch.append(pltpu.VMEM((2, tiles, width), f32))
            scratch.append(pltpu.VMEM((tiles, levels, LANES), f32))
            out_shape.append(mark)
            out_specs.append(vmem)
        return pl.pallas_call(
            functools.partial(forecast_kernel, field),
            out_shape=out_shape,
            in_specs=[vmem] * (11 + len(inputs)),
            out_specs=out_specs,
            scratch_shapes=scratch,
            compiler_params=params(10),
            cost_estimate=pl.CostEstimate(
                flops=40_000_000, bytes_accessed=3_000_000, transcendentals=0
            ),
            name=f"forecast_{field}",
        )(*prepared, before, after, diffusivity, mixing, cell, heads, *inputs)

    def exchanged(array):
        return lax.all_to_all(array, "member", split_axis=0, concat_axis=0, tiled=True)

    sent0, spill0, done0 = forecast(0, prepare(0), obs_index)
    held0 = exchanged(sent0)
    place, first, sea = pl.pallas_call(
        locate_kernel,
        out_shape=[
            pltpu.HBM((tiles, 2 * width), i32),
            pltpu.HBM((tiles, LANES), i32),
            pltpu.HBM((rows, width), f32),
        ],
        in_specs=[vmem, anywhere],
        out_specs=[vmem] * 3,
        compiler_params=params(8),
        cost_estimate=pl.CostEstimate(
            flops=20_000_000, bytes_accessed=500_000, transcendentals=0
        ),
        name="locate",
    )(mask, done0)
    sent1, spill1 = forecast(1, prepare(1, first))
    sent1, sums = pl.pallas_call(
        gram_kernel,
        out_shape=[bulks[1], mark],
        in_specs=[smem, vmem, vmem, vmem, smem, anywhere],
        out_specs=[anywhere, vmem],
        scratch_shapes=[
            pltpu.VMEM((tiles, 1, levels, LANES), f32),
            pltpu.SemaphoreType.DMA,
        ],
        input_output_aliases={5: 0},
        compiler_params=params(4),
        name="gram",
    )(tile.reshape(1).astype(jnp.int32), held0, obs_value, obs_error, obs_count, sent1)
    deep = members * levels
    halves = [pltpu.VMEM((deep, deep), jnp.bfloat16)] * 2

    def late(spill0, spill1, sums):
        there = exchanged(jnp.concatenate([spill0, spill1], axis=1))
        parts = exchanged(jnp.broadcast_to(sums[None, None], (members, 1, *sums.shape)))
        there = pl.pallas_call(
            spill_kernel,
            out_shape=jax.ShapeDtypeStruct(there.shape, f32),
            in_specs=[vmem] * 2,
            out_specs=vmem,
            scratch_shapes=halves,
            compiler_params=params(16),
            name="mix_spill",
        )(parts, there)
        there = exchanged(there)
        return there[:, :SPILL], there[:, SPILL:]

    def none(spill0, spill1, sums):
        return spill0, spill1

    most = pl.pallas_call(
        census_kernel,
        out_shape=jax.ShapeDtypeStruct((levels, LANES), f32),
        in_specs=[vmem, anywhere],
        out_specs=vmem,
        compiler_params=params(4),
        cost_estimate=pl.CostEstimate(
            flops=10_000_000, bytes_accessed=1_300_000, transcendentals=0
        ),
        name="census",
    )(land_mask, done0)
    spill0, spill1 = lax.cond(most[0, 0] > ROOM, late, none, spill0, spill1, sums)
    sent1, spill0, spill1 = lax.optimization_barrier((sent1, spill0, spill1))
    held1 = exchanged(sent1)

    updated = pl.pallas_call(
        mix_kernel,
        out_shape=jax.ShapeDtypeStruct((members, fields * PACKED, levels, LANES), f32),
        in_specs=[vmem, vmem],
        out_specs=vmem,
        scratch_shapes=halves,
        compiler_params=params(16),
        name="mix",
    )(held0, held1)
    back = exchanged(updated)

    bands = pl.BlockSpec((1, fields, levels, 16, width), lambda i: (0, 0, 0, i, 0))
    return pl.pallas_call(
        settle_kernel,
        grid=(rows // 16,),
        out_shape=jax.ShapeDtypeStruct(starting_tracer_fields.shape, f32),
        in_specs=[smem] + [vmem] * 6,
        out_specs=bands,
        compiler_params=params(12),
        name="settle",
    )(
        first, back.reshape(-1, levels, LANES), spill0, spill1, place, sea, starting_tracer_fields,
    )


def solution(mesh):
    placed = (
        P("member", None, None, "domain", None),
        P("member", None, "domain", None),
        P(),
        P(),
        P(),
        P("domain", None, None),
        P("domain", None),
        P("domain", None, None),
        P("domain", None, None),
    )
    return jax.shard_map(
        shards,
        mesh=mesh,
        in_specs=placed,
        out_specs=P("member", None, None, "domain", None),
        check_vma=False,
    )
```

```python
import functools

import jax
import jax.numpy as jnp
from jax import lax
from jax.experimental import pallas as pl
from jax.experimental.pallas import tpu as pltpu
from jax.sharding import PartitionSpec as P

FIELDS = 2
LEVELS = 8
LANES = 128
HALO = 2
UNROLL = 20
PACKED = 9
TAIL = 32
ROOM = PACKED * LANES - TAIL
SPILL = 2


def spread_row(row):
    return jnp.broadcast_to(row, (LEVELS, row.shape[1]))


def ranked(mask_ref, tiles, cells):
    rows = 2 * tiles
    blocks = cells // LANES
    sea = mask_ref[HALO : HALO + rows, :].astype(jnp.bfloat16)
    pick = lax.broadcasted_iota(jnp.int32, (tiles, rows), 1) - 2 * lax.broadcasted_iota(
        jnp.int32, (tiles, rows), 0
    )
    sides = [
        jnp.dot((pick == s).astype(jnp.bfloat16), sea, preferred_element_type=jnp.float32)
        for s in range(2)
    ]
    sea = jnp.concatenate(sides, axis=1)
    land = (1.0 - sea).astype(jnp.bfloat16)
    stacked = jnp.concatenate([land[:, b * LANES : (b + 1) * LANES] for b in range(blocks)], axis=0)
    before = (
        lax.broadcasted_iota(jnp.int32, (LANES, LANES), 0)
        < lax.broadcasted_iota(jnp.int32, (LANES, LANES), 1)
    ).astype(jnp.bfloat16)
    within = jnp.dot(stacked, before, preferred_element_type=jnp.float32)
    totals = jnp.dot(
        stacked, jnp.ones((LANES, LANES), jnp.bfloat16), preferred_element_type=jnp.float32
    )
    offset = jnp.zeros((tiles, LANES), jnp.float32)
    shifts = []
    for b in range(blocks):
        part = slice(b * tiles, (b + 1) * tiles)
        shifts.append(within[part] + offset)
        offset = offset + totals[part]
    return sea, jnp.concatenate(shifts, axis=1).astype(jnp.int32)


def placed_cells(sea, shift):
    rank = lax.broadcasted_iota(jnp.int32, shift.shape, 1) - shift
    place = jnp.where(rank < ROOM, rank, rank + TAIL)
    return place, jnp.where(sea > 0.0, place, -1)


def spilling(marked, shape):
    last = jnp.max(jnp.max(marked, axis=1, keepdims=True), axis=0, keepdims=True)
    return (jnp.broadcast_to(last, shape) >= PACKED * LANES).astype(jnp.int32)


def locate_kernel(mask_ref, _, place_ref, first_ref, sea_ref):
    tiles, cells = place_ref.shape
    sea_ref[...] = mask_ref[HALO : HALO + 2 * tiles, :]
    place, marked = placed_cells(*ranked(mask_ref, tiles, cells))
    place_ref[...] = marked
    lane = lax.broadcasted_iota(jnp.int32, first_ref.shape, 1)
    first = jnp.zeros(first_ref.shape, jnp.int32)
    for b in range(cells // LANES):
        head = place[:, b * LANES : b * LANES + 1]
        head = (jnp.minimum(head >> 7, PACKED - 1) << 7) + (head & (LANES - 1))
        first = jnp.where(lane == b, jnp.broadcast_to(head, first.shape), first)
    number = lax.broadcasted_iota(jnp.int32, first.shape, 0)
    first = first + number * (FIELDS * PACKED * LANES)
    first_ref[...] = jnp.where(lane == LANES - 1, spilling(marked, first.shape), first)


def survey_kernel(mask_ref, cell_ref, head_ref):
    tiles, cells = cell_ref.shape[0], 2 * mask_ref.shape[1]
    sea, shift = ranked(mask_ref, tiles, cells)
    cell = lax.broadcasted_iota(jnp.int32, shift.shape, 1)
    state = jnp.where(sea > 0.0, shift * 2048 + cell, 0)
    for bit in range(11):
        other = pltpu.roll(state, cells - (1 << bit), 1)
        comes = (other & (2048 << bit)) != 0
        goes = (state & (2048 << bit)) != 0
        state = jnp.where(comes, other, jnp.where(goes, 0, state))
    state = state & 2047
    heads = jnp.zeros(head_ref.shape, jnp.int32)
    lane = lax.broadcasted_iota(jnp.int32, heads.shape, 1)
    number = lax.broadcasted_iota(jnp.int32, heads.shape, 0)
    reach = jnp.zeros((tiles, 1), jnp.int32)
    for q in range(PACKED):
        part = state[:, q * LANES : (q + 1) * LANES]
        heads = jnp.where(lane == q, jnp.broadcast_to(part[:, 0:1], heads.shape), heads)
        reach = jnp.maximum(reach, jnp.max(part, axis=1, keepdims=True) - part[:, 0:1])
    wide = jnp.max(reach, axis=0, keepdims=True)
    heads = heads + number * cells
    heads = jnp.where(lane == PACKED, jnp.broadcast_to(wide, heads.shape), heads)
    _, marked = placed_cells(sea, shift)
    head_ref[...] = jnp.where(lane == PACKED + 1, spilling(marked, heads.shape), heads)
    state = state + lax.broadcasted_iota(jnp.int32, state.shape, 0) * cells
    cell_ref[:, : PACKED * LANES] = state[:, : PACKED * LANES]
    cell_ref[:, PACKED * LANES :] = pltpu.roll(state, cells - ROOM, 1)[:, : SPILL * LANES]


def prepare_kernel(field, x_ref, flux_ref, mask_ref, *rest):
    turned, wet, source, sea8, crowd8, held, sems = rest[-7:]
    rows, width = turned.shape[0], turned.shape[2]
    tall = rows + 2 * HALO
    parts = rows // 8
    copies = []
    for p in range(parts):
        span = pl.ds(p * 8, 8)
        copy = pltpu.make_async_copy(
            x_ref.at[0, field, :, span, :], held.at[:, span, :], sems.at[p]
        )
        copy.start()
        copies.append(copy)
    sea = mask_ref[1 : tall - 1, :]
    crowd = (
        mask_ref[0 : tall - 2, :] + mask_ref[2:tall, :]
        + pltpu.roll(sea, 1, 1) + pltpu.roll(sea, width - 1, 1)
    )
    for r in range(tall):
        sea8[r] = spread_row(mask_ref[r : r + 1, :])
    for r in range(1, tall - 1):
        crowd8[r] = spread_row(crowd[r - 1 : r, :])
    top = lax.broadcasted_iota(jnp.int32, (LEVELS, width), 0) == 0
    for p in range(parts):
        copies[p].wait()
        start = p * 8
        flipped = jnp.swapaxes(held[:, start : start + 8, :], 0, 1)
        for k in range(8):
            r = start + k
            turned[r] = flipped[k]
            wet[r] = flipped[k] * sea8[r + HALO]
            source[r] = jnp.where(top, spread_row(flux_ref[0, field, r : r + 1, :]), 0.0)


def forecast_kernel(field, turned, wet, source, sea8, crowd8, before_ref, after_ref,
                    diff_ref, mix_ref, *rest):
    cell_ref, head_ref, rest = rest[0], rest[1], rest[2:]
    if field == 0:
        index_ref, out_ref, spill_ref, done_ref, first, moist, plain, packed, heads, sems, surface, tails = rest
        done_ref[...] = jnp.zeros_like(done_ref)
    else:
        out_ref, spill_ref, first, moist, plain, packed, heads, sems = rest
    table = pltpu.make_async_copy(head_ref, heads, sems.at[0])
    table.start()
    rows, width = turned.shape[0], turned.shape[2]
    tall = rows + 2 * HALO
    blocks = width // LANES

    level = lax.broadcasted_iota(jnp.int32, (LEVELS, LEVELS), 0)
    lane = lax.broadcasted_iota(jnp.int32, (LEVELS, LEVELS), 1)
    diff = diff_ref[field : field + 1, :]
    mix = jnp.concatenate([mix_ref[field : field + 1, :], jnp.zeros((1, 1), jnp.float32)], axis=1)

    def along(table, shift):
        column = jnp.sum(jnp.where(lane + shift == level, table, 0.0), axis=1, keepdims=True)
        return jnp.concatenate([jnp.broadcast_to(column, (LEVELS, LANES))] * blocks, axis=1)

    lateral, above, below = along(diff, 0), along(mix, 0), along(mix, 1)
    vertical = above + below

    def stepped(r, x, y, north, south, gain):
        sea = sea8[r]
        around = north + south + pltpu.roll(y, 1, 1) + pltpu.roll(y, width - 1, 1)
        change = lateral * (around - crowd8[r] * x) - vertical * x + gain
        change = change + above * pltpu.roll(x, LEVELS - 1, 0)
        change = change + below * pltpu.roll(x, 1, 0)
        return x + sea * change

    def near(r):
        if r < HALO:
            x = before_ref[field, r * LEVELS : (r + 1) * LEVELS, :]
        elif r >= HALO + rows:
            h = r - HALO - rows
            x = after_ref[field, h * LEVELS : (h + 1) * LEVELS, :]
        else:
            return turned[r - HALO], wet[r - HALO]
        return x, x * sea8[r]

    top = lax.broadcasted_iota(jnp.int32, (LEVELS, width), 0) == 0

    def gain_at(r):
        if HALO <= r < HALO + rows:
            return source[r - HALO]
        ref = before_ref if r < HALO else after_ref
        line = ref[field, HALO * LEVELS : HALO * LEVELS + 1, :]
        return jnp.where(top, spread_row(line), 0.0)

    def keep(r, value):
        first[r] = value
        moist[r] = value * sea8[r]

    def inner(r, _):
        i = r - HALO
        keep(r, stepped(r, turned[i], wet[i], wet[i - 1], wet[i + 1], source[i]))
        return 0

    body = (tall - 6) // UNROLL * UNROLL
    for r in (1, 2, *range(3 + body, tall - 1)):
        x, y = near(r)
        keep(r, stepped(r, x, y, near(r - 1)[1], near(r + 1)[1], gain_at(r)))
    lax.fori_loop(3, 3 + body, inner, 0, unroll=UNROLL)

    def outer(tile, _):
        for side in range(2):
            r = HALO + 2 * tile + side
            value = stepped(r, first[r], moist[r], moist[r - 1], moist[r + 1], source[r - HALO])
            for j in range(blocks):
                plain[tile * 2 * blocks + side * blocks + j] = value[:, j * LANES : (j + 1) * LANES]
            if field == 0:
                surface[side, pl.ds(tile, 1), :] = value[0:1, :]
        return 0

    tiles = rows // 2
    lax.fori_loop(0, tiles, outer, 0, unroll=4)
    table.wait()
    lane_row = lax.broadcasted_iota(jnp.int32, (LEVELS, LANES), 1)

    def take(piece, lanes):
        return jnp.take_along_axis(piece, lanes, axis=1, mode="promise_in_bounds")

    if field == 0:
        slots = index_ref.shape[2]
        for g in range(tiles // 8):
            pieces = []
            for h in range(slots // LANES):
                where = index_ref[0, g * 8 : (g + 1) * 8, h * LANES : (h + 1) * LANES]
                block, lanes = where >> 7, where & (LANES - 1)
                found = jnp.zeros((8, LANES), jnp.float32)
                for q in range(2 * blocks):
                    s, j = divmod(q, blocks)
                    piece = surface[s, g * 8 : (g + 1) * 8, j * LANES : (j + 1) * LANES]
                    found = jnp.where(block == q, take(piece, lanes), found)
                for k in range(LANES // TAIL):
                    move = (LANES - TAIL - k * TAIL) % LANES
                    pieces.append(pltpu.roll(found, move, 1) if move else found)
            tails[g * 8 : (g + 1) * 8] = jnp.swapaxes(jnp.stack(pieces, axis=0), 0, 1)

    def wanted_at(base, t, q):
        row = cell_ref[pl.ds(base, 8), q * LANES : (q + 1) * LANES]
        return spread_row(row[t : t + 1])

    def chosen_from(tile, wanted, start):
        own = tile * 2 * blocks
        block, lanes = wanted >> 7, wanted & (LANES - 1)
        chosen = take(plain[own + start], lanes)
        for b in range(start + 1, 2 * blocks):
            chosen = jnp.where(block == own + b, take(plain[own + b], lanes), chosen)
        return chosen

    def sent(base, group):
        part = pl.ds(base, 8)
        return pltpu.make_async_copy(
            packed.at[part, pl.ds(0, PACKED)], out_ref.at[part, pl.ds(0, PACKED)], sems.at[group]
        )

    def pack(group, _, near):
        base = pl.multiple_of(group * 8, 8)
        for t in range(8):
            tile = base + t
            for q in range(PACKED):
                wanted = wanted_at(base, t, q)
                if near:
                    head = heads[tile, q]
                    b = head >> 7
                    turn = lane_row >= (head & (LANES - 1))
                    low, middle, high = plain[b], plain[b + 1], plain[b + 2]
                    lanes = wanted & (LANES - 1)
                    early = take(jnp.where(turn, low, middle), lanes)
                    late = take(jnp.where(turn, middle, high), lanes)
                    chosen = jnp.where(wanted - head < LANES, early, late)
                else:
                    chosen = chosen_from(tile, wanted, q)
                if field == 0 and q == PACKED - 1:
                    chosen = jnp.where(lane_row >= LANES - TAIL, tails[tile], chosen)
                packed[tile, q] = chosen
        sent(base, group).start()
        return 0

    groups = tiles // 8

    @pl.when(heads[0, PACKED] < 2 * LANES)
    def _():
        lax.fori_loop(0, groups, functools.partial(pack, near=True), 0)

    @pl.when(heads[0, PACKED] >= 2 * LANES)
    def _():
        lax.fori_loop(0, groups, functools.partial(pack, near=False), 0)

    @pl.when(heads[0, PACKED + 1] > 0)
    def _():
        def late_cells(group, _):
            base = pl.multiple_of(group * 8, 8)
            for t in range(8):
                for q in range(PACKED, PACKED + SPILL):
                    packed[base + t, q] = chosen_from(
                        base + t, wanted_at(base, t, q), ROOM // LANES
                    )
            return 0

        lax.fori_loop(0, groups, late_cells, 0)
        copy = pltpu.make_async_copy(
            packed.at[:, pl.ds(PACKED, SPILL)], spill_ref, sems.at[groups]
        )
        copy.start()
        copy.wait()

    for g in range(groups):
        sent(g * 8, g).wait()


def gram_kernel(
    tile_ref, held_ref, value_ref, error_ref, count_ref, _, out_ref, sums_ref, spread, sem
):
    tile = tile_ref[0]
    members = held_ref.shape[0]
    halves = value_ref.shape[2] // LANES
    slot = lax.broadcasted_iota(jnp.int32, (1, LANES), 1)
    total = jnp.zeros((members + 8, members), jnp.float32)
    for h in range(halves):
        seen = jnp.zeros((members, LANES), jnp.float32)
        for k in range(LANES // TAIL):
            piece = held_ref[:, PACKED - 1, h * (LANES // TAIL) + k, :]
            move = (k + 1) * TAIL % LANES
            piece = pltpu.roll(piece, move, 1) if move else piece
            seen = jnp.where((slot >= k * TAIL) & (slot < (k + 1) * TAIL), piece, seen)
        average = jnp.mean(seen, axis=0, keepdims=True)
        anomaly = seen - average
        span = slice(h * LANES, (h + 1) * LANES)
        own = lax.broadcasted_iota(jnp.int32, (value_ref.shape[1], LANES), 0) == tile
        value = jnp.sum(jnp.where(own, value_ref[0, :, span], 0.0), axis=0, keepdims=True)
        error = jnp.sum(jnp.where(own, error_ref[0, :, span], 0.0), axis=0, keepdims=True)
        active = jnp.where(slot + h * LANES < count_ref[0, tile], 1.0, 0.0)
        weight = active / error
        drift = weight * (value - average)
        left = jnp.concatenate([anomaly * weight, jnp.broadcast_to(drift, (8, LANES))], axis=0)
        total = total + lax.dot_general(
            left, anomaly, (((1,), (1,)), ((), ())),
            precision=lax.Precision.HIGHEST, preferred_element_type=jnp.float32,
        )
    packed = jnp.concatenate([total[g * 8 : (g + 1) * 8] for g in range(4)], axis=1)
    pull = jnp.concatenate([total[members : members + 8]] * 4, axis=1)
    row = lax.broadcasted_iota(jnp.int32, packed.shape, 0)
    lane = lax.broadcasted_iota(jnp.int32, packed.shape, 1)
    corner = (lane >= 16) & (lane < 32)
    packed = jnp.where(corner & (row == 0), pltpu.roll(pull, 16, 1), packed)
    packed = jnp.where(corner & (row == 1), pull, packed)
    sums_ref[...] = packed
    for m in range(members):
        spread[m, 0] = packed
    copy = pltpu.make_async_copy(spread, out_ref.at[:, pl.ds(PACKED, 1)], sem)
    copy.start()
    copy.wait()


def ensemble_kernel(packed, wide):
    count = 32
    lane = lax.broadcasted_iota(jnp.int32, (count, LANES), 1)
    row = lax.broadcasted_iota(jnp.int32, (count, LANES), 0)
    gram = jnp.concatenate(
        [packed if g == 0 else pltpu.roll(packed, LANES - g * count, 1) for g in range(4)], axis=0
    )
    pull = jnp.where(
        lane[0:1] < 16,
        pltpu.roll(packed[0:8], LANES - 16, 1)[0:1],
        packed[1:2],
    )
    gram = gram + jnp.where(lane == row, count - 1.0, 0.0)
    columns = [jnp.broadcast_to(gram[:, k : k + 1], (count, LANES)) for k in range(count)]
    work = jnp.where(lane == row, 1.0, 0.0)
    for k in range(count):
        base = (k // 8) * 8
        column = columns[k][base:]
        pivot = jnp.broadcast_to(column[k - base : k - base + 1], (8, LANES))
        scale = lax.rsqrt(pivot)
        scale = scale * (1.5 - 0.5 * pivot * scale * scale)
        head = scale[0:1]
        lead = work[k : k + 1] * head
        column = column * head
        below = row[base:] > k
        factor = jnp.where(below, column, 0.0)
        rest = jnp.where(row[base:] == k, lead, work[base:] - factor * lead)
        work = rest if base == 0 else jnp.concatenate([work[:base], rest], axis=0)
        for c in range(k + 1, count):
            cbase = (c // 8) * 8
            ratio = column[c - base : c - base + 1]
            old = columns[c]
            fresh = old[cbase:] - column[cbase - base :] * ratio
            columns[c] = fresh if cbase == 0 else jnp.concatenate([old[:cbase], fresh], axis=0)
    inverse = work
    gained = jnp.sum(inverse * pull, axis=1, keepdims=True)
    mean_weight = jnp.sum(inverse * gained, axis=0, keepdims=True)
    live = lane < count
    weights = jnp.where(live, mean_weight + jnp.sqrt(count - 1.0) * inverse, 0.0)
    centre = jnp.sum(weights, axis=1, keepdims=True) * (1.0 / count)
    return jnp.where(live, weights - centre + 1.0 / count, 0.0)


def mixed(high, low, data):
    major = data.astype(jnp.bfloat16)
    minor = (data - major.astype(jnp.float32)).astype(jnp.bfloat16)
    total = jnp.dot(high[...], major, preferred_element_type=jnp.float32)
    total = total + jnp.dot(high[...], minor, preferred_element_type=jnp.float32)
    return total + jnp.dot(low[...], major, preferred_element_type=jnp.float32)


def mix_strip(high, low, data_ref, at, out_ref, to, blocks):
    members = data_ref.shape[0]
    deep = members * LEVELS
    data = jnp.concatenate(
        [data_ref[:, at + b].reshape(deep, LANES) for b in range(blocks)], axis=1
    )
    result = mixed(high, low, data)
    for b in range(blocks):
        out_ref[:, to + b] = result[:, b * LANES : (b + 1) * LANES].reshape(members, LEVELS, LANES)


def widen(total, high, low):
    members = total.shape[1] // 4
    deep = members * LEVELS
    kernel = ensemble_kernel(total, LANES)[:, :members]
    major = kernel.astype(jnp.bfloat16)
    minor = (kernel - major.astype(jnp.float32)).astype(jnp.bfloat16)
    spread = (
        lax.broadcasted_iota(jnp.int32, (deep, members), 0) // LEVELS
        == lax.broadcasted_iota(jnp.int32, (deep, members), 1)
    ).astype(jnp.bfloat16)
    same = (
        lax.broadcasted_iota(jnp.int32, (deep, deep), 0) % LEVELS
        == lax.broadcasted_iota(jnp.int32, (deep, deep), 1) % LEVELS
    )
    for part, target in ((major, high), (minor, low)):
        tall = jnp.dot(spread, part, preferred_element_type=jnp.float32).astype(jnp.bfloat16)
        full = lax.dot_general(
            tall, spread, (((1,), (1,)), ((), ())), preferred_element_type=jnp.float32
        )
        target[...] = jnp.where(same, full, 0.0).astype(jnp.bfloat16)


def mix_kernel(data0_ref, data1_ref, out_ref, high, low):
    widen(jnp.sum(data1_ref[:, PACKED], axis=0), high, low)
    blocks = PACKED
    for f, data_ref in ((0, data0_ref), (1, data1_ref)):

        def strip(i, _, f=f, data_ref=data_ref):
            at = i * blocks
            mix_strip(high, low, data_ref, at, out_ref, f * PACKED + at, blocks)
            return 0

        lax.fori_loop(0, PACKED // blocks, strip, 0)


def spill_kernel(sums_ref, data_ref, out_ref, high, low):
    widen(jnp.sum(sums_ref[:, 0], axis=0), high, low)
    mix_strip(high, low, data_ref, 0, out_ref, 0, data_ref.shape[1])


def census_kernel(mask_ref, _, most_ref):
    rows = jnp.sum(mask_ref[...].astype(jnp.float32), axis=1, keepdims=True)
    rows = jnp.broadcast_to(rows, (rows.shape[0], LANES))
    pairs = rows + pltpu.roll(rows, rows.shape[0] - 1, 0)
    even = lax.broadcasted_iota(jnp.int32, pairs.shape, 0) % 2 == 0
    most = jnp.max(jnp.where(even, pairs, 0.0), axis=0, keepdims=True)
    most_ref[...] = jnp.broadcast_to(most, most_ref.shape)


def settle_rows(
    spilled, first_ref, back_ref, spill0_ref, spill1_ref, place_ref, sea_ref, x_ref, out_ref
):
    blocks = out_ref.shape[4] // LANES
    start = pl.multiple_of(pl.program_id(0) * 8, 8)
    end = back_ref.shape[0] - 1
    lane_row = lax.broadcasted_iota(jnp.int32, (LEVELS, LANES), 1)

    def take(source, lanes):
        return jnp.take_along_axis(source, lanes, axis=1, mode="promise_in_bounds")

    for j in range(blocks):
        lanes_at = slice(j * LANES, (j + 1) * LANES)
        wanted8 = [
            place_ref[pl.ds(start, 8), b * LANES : (b + 1) * LANES] for b in (j, blocks + j)
        ]
        for half in range(2):
            rows = ([], [])
            for t in range(half * 4, half * 4 + 4):
                for s in range(2):
                    b = s * blocks + j
                    wanted = spread_row(wanted8[s][t : t + 1])
                    block, lanes = wanted >> 7, wanted & (LANES - 1)
                    head = first_ref[start + t, b]
                    at = head >> 7
                    turn = lane_row >= (head & (LANES - 1))
                    for f in range(FIELDS):
                        low = back_ref[at + f * PACKED]
                        high = back_ref[jnp.minimum(at + (f * PACKED + 1), end)]
                        value = take(jnp.where(turn, low, high), lanes)
                        if spilled and (b + 1) * LANES > ROOM:
                            for o in range(SPILL):
                                late = take((spill0_ref, spill1_ref)[f][start + t, o], lanes)
                                value = jnp.where(block == PACKED + o, late, value)
                        rows[f].append(value)
            here = pl.ds(pl.multiple_of(2 * start + half * 8, 8), 8)
            there = slice(half * 8, half * 8 + 8)
            ocean = sea_ref[here, lanes_at] > 0.0
            for f in range(FIELDS):
                turned = jnp.swapaxes(jnp.stack(rows[f], axis=0), 0, 1)
                for l in range(LEVELS):
                    out_ref[0, f, l, there, lanes_at] = jnp.where(
                        ocean, turned[l], x_ref[0, f, l, here, lanes_at]
                    )


def settle_kernel(first_ref, *refs):
    late = first_ref[0, LANES - 1] > 0

    @pl.when(late)
    def _():
        settle_rows(True, first_ref, *refs)

    @pl.when(jnp.logical_not(late))
    def _():
        settle_rows(False, first_ref, *refs)


def shards(
    starting_tracer_fields,
    surface_exchange_inputs,
    diffusivity,
    mixing,
    land_mask,
    obs_index,
    obs_count,
    obs_value,
    obs_error,
):
    _, fields, levels, rows, width = starting_tracer_fields.shape
    members = lax.axis_size("member")
    domains = lax.axis_size("domain")
    blocks = width // LANES
    tiles = members
    per_field = 2 * blocks
    tile = lax.axis_index("member")
    domain = lax.axis_index("domain")
    state, flux = starting_tracer_fields[0], surface_exchange_inputs[0]

    def edge(first, flux_row):
        lines = jnp.swapaxes(state[:, :, first : first + HALO], 1, 2)
        lines = lines.reshape(fields, HALO * levels, width)
        return jnp.concatenate([lines, flux[:, flux_row : flux_row + 1]], axis=1)

    up = [(i, i + 1) for i in range(domains - 1)]
    down = [(i + 1, i) for i in range(domains - 1)]
    before = lax.ppermute(edge(rows - HALO, rows - 1), "domain", up)
    after = lax.ppermute(edge(0, 0), "domain", down)

    padded = jnp.pad(land_mask, ((HALO, HALO), (0, 0)))
    mask = lax.dynamic_slice_in_dim(padded, domain * rows, rows + 2 * HALO, 0).astype(jnp.float32)

    f32 = jnp.float32
    tall = rows + 2 * HALO
    vmem = pl.BlockSpec(memory_space=pltpu.VMEM)
    smem = pl.BlockSpec(memory_space=pltpu.SMEM)
    anywhere = pl.BlockSpec(memory_space=pl.ANY)
    hbm = pl.BlockSpec(memory_space=pltpu.HBM)

    def params(mib):
        return pltpu.CompilerParams(vmem_limit_bytes=mib << 20)

    band = jax.ShapeDtypeStruct((rows, levels, width), f32)
    shell = jax.ShapeDtypeStruct((tall, levels, width), f32)
    i32 = jnp.int32
    bulks = [
        pltpu.HBM((tiles, PACKED, levels, LANES), f32),
        jax.ShapeDtypeStruct((tiles, PACKED + 1, levels, LANES), f32),
    ]
    extra = pltpu.HBM((tiles, SPILL, levels, LANES), f32)
    mark = jax.ShapeDtypeStruct((levels, LANES), f32)

    cell, heads = pl.pallas_call(
        survey_kernel,
        out_shape=[
            jax.ShapeDtypeStruct((tiles, (PACKED + SPILL) * LANES), i32),
            jax.ShapeDtypeStruct((tiles, LANES), i32),
        ],
        in_specs=[vmem],
        out_specs=[vmem] * 2,
        compiler_params=params(8),
        cost_estimate=pl.CostEstimate(
            flops=20_000_000, bytes_accessed=500_000, transcendentals=0
        ),
        name="survey",
    )(mask)

    def prepare(field, *after_this):
        return pl.pallas_call(
            functools.partial(prepare_kernel, field),
            out_shape=[band, band, band, shell, shell],
            in_specs=[hbm, vmem, vmem] + [anywhere] * len(after_this),
            out_specs=[vmem] * 5,
            scratch_shapes=[
                pltpu.VMEM((levels, rows, width), f32),
                pltpu.SemaphoreType.DMA((rows // 8,)),
            ],
            compiler_params=params(8),
            cost_estimate=pl.CostEstimate(
                flops=20_000_000, bytes_accessed=3_000_000, transcendentals=0
            ),
            name=f"prepare_{field}",
        )(
            pltpu.with_memory_space_constraint(starting_tracer_fields, pltpu.HBM),
            surface_exchange_inputs, mask, *after_this,
        )

    def forecast(field, prepared, *inputs):
        scratch = [
            pltpu.VMEM((tall, levels, width), f32),
            pltpu.VMEM((tall, levels, width), f32),
            pltpu.VMEM((tiles * per_field + 2, levels, LANES), f32),
            pltpu.VMEM((tiles, PACKED + SPILL, levels, LANES), f32),
            pltpu.SMEM((tiles, LANES), i32),
            pltpu.SemaphoreType.DMA((tiles // 8 + 1,)),
        ]
        out_shape = [bulks[field], extra]
        out_specs = [hbm if field == 0 else anywhere, hbm]
        if field == 0:
            scratch.append(pltpu.VMEM((2, tiles, width), f32))
            scratch.append(pltpu.VMEM((tiles, levels, LANES), f32))
            out_shape.append(mark)
            out_specs.append(vmem)
        return pl.pallas_call(
            functools.partial(forecast_kernel, field),
            out_shape=out_shape,
            in_specs=[vmem] * (11 + len(inputs)),
            out_specs=out_specs,
            scratch_shapes=scratch,
            compiler_params=params(10),
            cost_estimate=pl.CostEstimate(
                flops=40_000_000, bytes_accessed=3_000_000, transcendentals=0
            ),
            name=f"forecast_{field}",
        )(*prepared, before, after, diffusivity, mixing, cell, heads, *inputs)

    def exchanged(array):
        return lax.all_to_all(array, "member", split_axis=0, concat_axis=0, tiled=True)

    sent0, spill0, done0 = forecast(0, prepare(0), obs_index)
    held0 = exchanged(sent0)
    place, first, sea = pl.pallas_call(
        locate_kernel,
        out_shape=[
            pltpu.HBM((tiles, 2 * width), i32),
            pltpu.HBM((tiles, LANES), i32),
            pltpu.HBM((rows, width), f32),
        ],
        in_specs=[vmem, anywhere],
        out_specs=[vmem] * 3,
        compiler_params=params(8),
        cost_estimate=pl.CostEstimate(
            flops=20_000_000, bytes_accessed=500_000, transcendentals=0
        ),
        name="locate",
    )(mask, done0)
    sent1, spill1 = forecast(1, prepare(1, first))
    sent1, sums = pl.pallas_call(
        gram_kernel,
        out_shape=[bulks[1], mark],
        in_specs=[smem, vmem, vmem, vmem, smem, anywhere],
        out_specs=[anywhere, vmem],
        scratch_shapes=[
            pltpu.VMEM((tiles, 1, levels, LANES), f32),
            pltpu.SemaphoreType.DMA,
        ],
        input_output_aliases={5: 0},
        compiler_params=params(4),
        name="gram",
    )(tile.reshape(1).astype(jnp.int32), held0, obs_value, obs_error, obs_count, sent1)
    deep = members * levels
    halves = [pltpu.VMEM((deep, deep), jnp.bfloat16)] * 2

    def late(spill0, spill1, sums):
        there = exchanged(jnp.concatenate([spill0, spill1], axis=1))
        parts = exchanged(jnp.broadcast_to(sums[None, None], (members, 1, *sums.shape)))
        there = pl.pallas_call(
            spill_kernel,
            out_shape=jax.ShapeDtypeStruct(there.shape, f32),
            in_specs=[vmem] * 2,
            out_specs=vmem,
            scratch_shapes=halves,
            compiler_params=params(16),
            name="mix_spill",
        )(parts, there)
        there = exchanged(there)
        return there[:, :SPILL], there[:, SPILL:]

    def none(spill0, spill1, sums):
        return spill0, spill1

    most = pl.pallas_call(
        census_kernel,
        out_shape=jax.ShapeDtypeStruct((levels, LANES), f32),
        in_specs=[vmem, anywhere],
        out_specs=vmem,
        compiler_params=params(4),
        cost_estimate=pl.CostEstimate(
            flops=10_000_000, bytes_accessed=1_300_000, transcendentals=0
        ),
        name="census",
    )(land_mask, done0)
    spill0, spill1 = lax.cond(most[0, 0] > ROOM, late, none, spill0, spill1, sums)
    sent1, spill0, spill1 = lax.optimization_barrier((sent1, spill0, spill1))
    held1 = exchanged(sent1)

    updated = pl.pallas_call(
        mix_kernel,
        out_shape=jax.ShapeDtypeStruct((members, fields * PACKED, levels, LANES), f32),
        in_specs=[vmem, vmem],
        out_specs=vmem,
        scratch_shapes=halves,
        compiler_params=params(16),
        name="mix",
    )(held0, held1)
    back = exchanged(updated)

    bands = pl.BlockSpec((1, fields, levels, 16, width), lambda i: (0, 0, 0, i, 0))
    return pl.pallas_call(
        settle_kernel,
        grid=(rows // 16,),
        out_shape=jax.ShapeDtypeStruct(starting_tracer_fields.shape, f32),
        in_specs=[smem] + [vmem] * 6,
        out_specs=bands,
        compiler_params=params(12),
        name="settle",
    )(
        first, back.reshape(-1, levels, LANES), spill0, spill1, place, sea, starting_tracer_fields,
    )


def solution(mesh):
    placed = (
        P("member", None, None, "domain", None),
        P("member", None, "domain", None),
        P(),
        P(),
        P(),
        P("domain", None, None),
        P("domain", None),
        P("domain", None, None),
        P("domain", None, None),
    )
    return jax.shard_map(
        shards,
        mesh=mesh,
        in_specs=placed,
        out_specs=P("member", None, None, "domain", None),
        check_vma=False,
    )
```
